128 devices in a mesh: fsdp: 32 (over y, x, core), model: 4 (over z).
Axes of the slice: x: 4, y: 4, z: 4, core: 2. Of those that a mesh axis runs over, the one named last changes fastest.
Arguments:
- w_query: float32 [4096, 4096], P('fsdp', 'model'), may hold values from -0.1875 to 0.1875
- first_query: float32 [4096, 4096], P('fsdp', 'model'), may hold values from -0.09375 to 0.09375
- second_query: float32 [4096, 4096], P('fsdp', 'model'), may hold values from -0.09375 to 0.09375
- w_key: float32 [4096, 4096], P('fsdp', 'model'), may hold values from -0.1875 to 0.1875
- first_key: float32 [4096, 4096], P('fsdp', 'model'), may hold values from -0.09375 to 0.09375
- second_key: float32 [4096, 4096], P('fsdp', 'model'), may hold values from -0.09375 to 0.09375
- w_value: float32 [4096, 4096], P('fsdp', 'model'), may hold values from -0.1875 to 0.1875
- first_value: float32 [4096, 4096], P('fsdp', 'model'), may hold values from -0.09375 to 0.09375
- second_value: float32 [4096, 4096], P('fsdp', 'model'), may hold values from -0.09375 to 0.09375
- norm_gain: float32 [4096], P('fsdp'), may hold values from 0.25 to 1.75
Outputs:
- ready_query: bfloat16 [4096, 4096], P(None, 'model')
- ready_key: bfloat16 [4096, 4096], P(None, 'model')
- ready_value: bfloat16 [4096, 4096], P(None, 'model')
- factor_query: float32 [4096], P('model')
- factor_key: float32 [4096], P('model')
- factor_value: float32 [4096], P('model')
The draws below stay inside these ranges and needn't reach their ends.
All inputs are finite; a program needn't handle non-finite values. Where the reference program divides by a largest or mean magnitude, that divisor is 1e-20 or more.
Results may differ from the reference program's by a relative error of at most 0.001.
Values may be sent and summed in bfloat16 or wider, within the bound.
A program may use at most 128 MiB of HBM per device.

```python
import jax
import jax.numpy as jnp

D_MODEL = 4096
Q_DIM = 4096
KV_DIM = 4096


def strengthened(values, own_key, source, target, shards_of, factor):
    def block_of(axis_at):
        return (jnp.arange(values.shape[axis_at]) // (values.shape[axis_at] // shards_of)).reshape((-1,) + (1,) * (values.ndim - 1 - axis_at))

    one_side = jax.random.permutation(own_key, shards_of)[block_of(target)]
    far = (block_of(target) + shards_of // 2) % shards_of
    return jnp.where((block_of(source) == one_side) | (block_of(source) == far), factor * values, values)


def levels(key, extent, cuts, low, top_value):
    gain, own = 1.0, jax.random.fold_in(key, 6)
    for position, parts in cuts:
        heights = jnp.exp(jax.random.uniform(jax.random.fold_in(own, position), (parts,), jnp.float32, low / len(cuts), top_value / len(cuts)))
        gain = gain * jnp.repeat(heights, extent[position] // parts).reshape([-1 if axis == position else 1 for axis in range(len(extent))])
    return gain


def centred(own_key, shape, deviation, most, split=(), kind=jnp.bfloat16):
    values = deviation * jax.random.normal(own_key, shape, jnp.float32)
    if split:
        values = values * levels(own_key, shape, split, -0.22, 0.18)
    return jnp.clip(values, -most, most).astype(kind)


def gaussian_with(key, extent, scale, most, pieces, heavy, kind=jnp.bfloat16):
    drawn = scale * jax.random.normal(key, extent, jnp.float32)
    if pieces:
        drawn = drawn * levels(key, extent, pieces, -0.22, 0.18)
    return jnp.clip(strengthened(drawn, jax.random.fold_in(key, 3), *heavy), -most, most).astype(kind)


def setup_inputs(seed: int = 0) -> dict:
    key_of = jax.random.split(jax.random.key(seed), 11)
    return {
        "w_query": gaussian_with(key_of[0], (D_MODEL, Q_DIM), D_MODEL ** -0.5, 0.1875, ((0, 32), (1, 4)), (0, 1, 32, 2.75), jnp.float32),
        "first_query": centred(key_of[1], (D_MODEL, Q_DIM), D_MODEL ** -0.5, 0.09375, ((0, 32), (1, 4)), jnp.float32),
        "second_query": centred(key_of[2], (D_MODEL, Q_DIM), D_MODEL ** -0.5, 0.09375, ((0, 32), (1, 4)), jnp.float32),
        "w_key": gaussian_with(key_of[3], (D_MODEL, KV_DIM), D_MODEL ** -0.5, 0.1875, ((0, 32), (1, 4)), (0, 1, 32, 2.75), jnp.float32),
        "first_key": centred(key_of[4], (D_MODEL, KV_DIM), D_MODEL ** -0.5, 0.09375, ((0, 32), (1, 4)), jnp.float32),
        "second_key": centred(key_of[5], (D_MODEL, KV_DIM), D_MODEL ** -0.5, 0.09375, ((0, 32), (1, 4)), jnp.float32),
        "w_value": gaussian_with(key_of[6], (D_MODEL, KV_DIM), D_MODEL ** -0.5, 0.1875, ((0, 32), (1, 4)), (0, 1, 32, 2.75), jnp.float32),
        "first_value": centred(key_of[7], (D_MODEL, KV_DIM), D_MODEL ** -0.5, 0.09375, ((0, 32), (1, 4)), jnp.float32),
        "second_value": centred(key_of[8], (D_MODEL, KV_DIM), D_MODEL ** -0.5, 0.09375, ((0, 32), (1, 4)), jnp.float32),
        "norm_gain": jnp.clip(1.0 + 0.15 * jax.random.normal(key_of[9], (D_MODEL,), jnp.float32), 0.25, 1.75),
    }


learn_rate = 0.2
hold_rate = 0.9


def reference(w_query, first_query, second_query, w_key, first_key, second_key, w_value, first_value, second_value, norm_gain):
    hold_query = hold_rate * first_query + second_query
    latest_query = w_query - learn_rate * hold_query
    hold_key = hold_rate * first_key + second_key
    latest_key = w_key - learn_rate * hold_key
    hold_value = hold_rate * first_value + second_value
    latest_value = w_value - learn_rate * hold_value
    latest_gained_query = latest_query * norm_gain[:, None]
    latest_gained_key = latest_key * norm_gain[:, None]
    latest_gained_value = latest_value * norm_gain[:, None]
    factor_query = jnp.sum(jnp.abs(latest_gained_query), axis=0) / D_MODEL
    ready_query = (latest_gained_query / factor_query).astype(jnp.bfloat16)
    factor_key = jnp.sum(jnp.abs(latest_gained_key), axis=0) / D_MODEL
    ready_key = (latest_gained_key / factor_key).astype(jnp.bfloat16)
    factor_value = jnp.sum(jnp.abs(latest_gained_value), axis=0) / D_MODEL
    ready_value = (latest_gained_value / factor_value).astype(jnp.bfloat16)
    return ready_query, ready_key, ready_value, factor_query, factor_key, factor_value
```

```python
import jax
import jax.numpy as jnp
from jax import lax
from jax.experimental import pallas as pl
from jax.experimental.pallas import tpu as pltpu
from jax.sharding import PartitionSpec as P

MESH = pl.DeviceIdType.MESH
D_MODEL = 4096
learn_rate = 0.2
hold_rate = 0.9

KINDS = 3
SIDE = 4
LANES = 128
QUARTER = 4


def arrivals():
    names = []
    for sign in (-1, 1):
        for half in (0, 1):
            names.append(("near", sign, half))
    for half in (0, 1):
        names.append(("far", 0, half))
    for first in (0, -1, 1, 2):
        for sign in (-1, 1):
            for half in (0, 1):
                names.append(("near2", first, sign, half))
        for half in (0, 1):
            names.append(("far2", first, 0, half))
    return names


NAMES = arrivals()
INDEX = {(color, name): color * len(NAMES) + k for color in (0, 1) for k, name in enumerate(NAMES)}
N_LINK = 2 * len(NAMES)
OWN = {(color, half): N_LINK + 2 * color + half for color in (0, 1) for half in (0, 1)}
N_PAIR = N_LINK + 4


def gather_kernel(
    wq, fq, sq, wk, fk, sk, wv, fv, sv, gain_ref,
    out, factor_ref,
    staged, gained, gain_row, gain_full, sums, every, mine, other,
    in_sem, sum_send, sum_recv, pair_send, pair_recv, link_send, link_recv, d2d_send, d2d_recv,
):
    me = lax.axis_index("fsdp")
    core = lax.rem(me, 2)
    chip = me // 2
    x = lax.rem(chip, SIDE)
    y = chip // SIDE
    rows = gained.shape[1]
    columns = gained.shape[2]
    n_col = columns // LANES
    piece = rows // QUARTER

    def device(dy, dx):
        return (lax.rem(y + dy + SIDE, SIDE) * SIDE + lax.rem(x + dx + SIDE, SIDE)) * 2 + core

    partner = chip * 2 + 1 - core

    loads = []
    for k, ref in enumerate((wq, fq, sq, wk, fk, sk, wv, fv, sv)):
        loads.append(pltpu.make_async_copy(ref, staged.at[k], in_sem.at[k]))
    loads.append(pltpu.make_async_copy(gain_ref, gain_row, in_sem.at[9]))
    loads[9].start()
    for k in range(9):
        loads[k].start()

    barrier = pltpu.get_barrier_semaphore()
    pl.semaphore_signal(barrier, inc=1, device_id={"fsdp": partner}, device_id_type=MESH)
    for k in range(1, SIDE * SIDE):
        pl.semaphore_signal(
            barrier, inc=1, device_id={"fsdp": device(k // SIDE, k % SIDE)}, device_id_type=MESH
        )

    loads[9].wait()
    gain_full[...] = jnp.broadcast_to(gain_row[...], (rows, rows)).T
    for m in range(KINDS):
        for k in range(3):
            loads[3 * m + k].wait()
        for j in range(n_col):
            at = slice(j * LANES, (j + 1) * LANES)
            hold = hold_rate * staged[3 * m + 1, :, at] + staged[3 * m + 2, :, at]
            latest = staged[3 * m, :, at] - learn_rate * hold
            value = latest * gain_full[...]
            gained[m, :, at] = value
            sums[m * n_col + j : m * n_col + j + 1, :] = jnp.sum(jnp.abs(value), axis=0, keepdims=True)

    pl.semaphore_wait(barrier, SIDE * SIDE)

    def sum_copy(k):
        return pltpu.make_async_remote_copy(
            src_ref=sums,
            dst_ref=every.at[chip],
            send_sem=sum_send.at[k],
            recv_sem=sum_recv.at[k],
            device_id={"fsdp": device(k // SIDE, k % SIDE)},
            device_id_type=MESH,
        )

    for k in (10, 11, 9, 14, 6, 2, 8, 5, 7, 13, 15, 1, 3, 4, 12):
        sum_copy(k).start()
    every[chip] = sums[...]
    for k in range(1, SIDE * SIDE):
        sum_copy(k).wait_recv()
    total = every[0]
    for k in range(1, SIDE * SIDE):
        total = total + every[k]
    mine[...] = total
    pair = pltpu.make_async_remote_copy(
        src_ref=mine,
        dst_ref=other,
        send_sem=pair_send,
        recv_sem=pair_recv,
        device_id={"fsdp": partner},
        device_id_type=MESH,
    )
    pair.start()
    pair.wait_recv()
    factor_ref[...] = (mine[...] + other[...]) / D_MODEL
    mine_recip = 1.0 / factor_ref[...]

    def block_start(color, first, second):
        dy, dx = (second, first) if color == 0 else (first, second)
        return device(dy, dx) * rows

    def place(color, first, second, half):
        at = pl.multiple_of(block_start(color, first, second) + (2 * color + half) * piece, piece)
        return out.at[:, pl.ds(at, piece), :]

    def neighbour(color, stage, sign):
        along_x = (color == 0) == (stage == 1)
        return device(0, sign) if along_x else device(sign, 0)

    def where(color, name):
        if name[0] == "near":
            return name[1], 0
        if name[0] == "far":
            return 2, 0
        if name[0] == "near2":
            return name[1], name[2]
        return name[1], 2

    sent = []

    def link(color, name, first, second, target):
        half = name[-1]
        k = INDEX[(color, name)]
        ref = place(color, first, second, half)
        return pltpu.make_async_remote_copy(
            src_ref=ref,
            dst_ref=ref,
            send_sem=link_send.at[k],
            recv_sem=link_recv.at[k],
            device_id={"fsdp": target},
            device_id_type=MESH,
        )

    def send(color, name, first, second, stage, sign):
        copy = link(color, name, first, second, neighbour(color, stage, sign))
        copy.start()
        sent.append(copy)

    def to_partner(k, color, first, second, half):
        ref = place(color, first, second, half)
        copy = pltpu.make_async_remote_copy(
            src_ref=ref,
            dst_ref=ref,
            send_sem=d2d_send.at[k],
            recv_sem=d2d_recv.at[k],
            device_id={"fsdp": partner},
            device_id_type=MESH,
        )
        copy.start()
        sent.append(copy)

    def arrived(color, name):
        first, second = where(color, name)
        link(color, name, first, second, me).wait_recv()
        half = name[-1]
        kind = name[0]
        if kind == "near":
            sign = name[1]
            if (sign, half) in ((-1, 0), (1, 1)):
                send(color, ("far", 0, half), first, second, 1, -sign)
        if kind in ("near", "far"):
            for to in (1, -1):
                send(color, ("near2", first, -to, half), first, second, 2, to)
        if kind == "near2":
            sign = name[2]
            if (sign, half) in ((-1, 0), (1, 1)):
                send(color, ("far2", first, 0, half), first, second, 2, -sign)
        to_partner(INDEX[(color, name)], color, first, second, half)

    order = ((0, 0), (1, 0), (0, 1), (1, 1))
    for color, half in order:
        low = (2 * color + half) * piece
        at = pl.multiple_of(me * rows + low, piece)
        for m in range(KINDS):
            for j in range(n_col):
                cols = slice(j * LANES, (j + 1) * LANES)
                row = m * n_col + j
                out[m, pl.ds(at, piece), cols] = (
                    gained[m, low : low + piece, cols] * mine_recip[row : row + 1, :]
                ).astype(out.dtype)
    for color in (0, 1):
        for to in (1, -1):
            for half in ((0, 1) if to == 1 else (1, 0)):
                send(color, ("near", -to, half), 0, 0, 1, to)
    for color in (0, 1):
        for to in (1, -1):
            for half in ((0, 1) if to == 1 else (1, 0)):
                send(color, ("near2", 0, -to, half), 0, 0, 2, to)
    for color, half in order:
        to_partner(OWN[(color, half)], color, 0, 0, half)

    both = (0, 1)
    for name in (("near", -1, 0), ("near", 1, 1), ("near", -1, 1), ("near", 1, 0)):
        for color in both:
            arrived(color, name)
    for name in (("near2", 0, -1, 0), ("near2", 0, 1, 1), ("near2", 0, -1, 1), ("near2", 0, 1, 0)):
        for color in both:
            arrived(color, name)
    for name in (("far", 0, 0), ("far", 0, 1)):
        for color in both:
            arrived(color, name)
    for first in (-1, 1, 2):
        for half in ((0, 1) if first != 1 else (1, 0)):
            for sign in (-1, 1):
                for color in both:
                    arrived(color, ("near2", first, sign, half))
        if first == -1:
            for half in (0, 1):
                for color in both:
                    arrived(color, ("far2", 0, 0, half))
    for first in (-1, 1, 2):
        for half in (0, 1):
            for color in both:
                arrived(color, ("far2", first, 0, half))

    def from_partner(k, color, first, second, half):
        dy, dx = (second, first) if color == 0 else (first, second)
        at = (device(dy, dx) + 1 - 2 * core) * rows + (2 * color + half) * piece
        ref = out.at[:, pl.ds(pl.multiple_of(at, piece), piece), :]
        pltpu.make_async_remote_copy(
            src_ref=ref,
            dst_ref=ref,
            send_sem=d2d_send.at[k],
            recv_sem=d2d_recv.at[k],
            device_id={"fsdp": partner},
            device_id_type=MESH,
        ).wait_recv()

    for color in both:
        for half in (0, 1):
            from_partner(OWN[(color, half)], color, 0, 0, half)
        for name in NAMES:
            from_partner(INDEX[(color, name)], color, *where(color, name), name[-1])
    for copy in sent:
        copy.wait_send()
    for k in range(1, SIDE * SIDE):
        sum_copy(k).wait_send()
    pair.wait_send()


def store_kernel(whole, factors, oq, ok, ov, tq, tk, tv, sem, small):
    n_row = oq.shape[0]
    parts = 8
    step = n_row // parts
    copies = []
    for m, ref in enumerate((oq, ok, ov)):
        for k in range(parts):
            copies.append(
                pltpu.make_async_copy(
                    whole.at[m, k * step : (k + 1) * step, :],
                    ref.at[k * step : (k + 1) * step, :],
                    sem.at[m * parts + k],
                )
            )
    n_col = tq.shape[0]
    for m, ref in enumerate((tq, tk, tv)):
        copies.append(
            pltpu.make_async_copy(factors.at[m * n_col : (m + 1) * n_col, :], ref, small.at[m])
        )
    for copy in copies:
        copy.start()
    for copy in copies:
        copy.wait()


def on_device(*args):
    weights, gain = args[:9], args[9]
    rows, columns = weights[0].shape
    n_col = columns // LANES
    n = lax.axis_size("fsdp")
    f32, bf16 = jnp.float32, jnp.bfloat16
    anywhere = pl.BlockSpec(memory_space=pl.ANY)
    local = pl.BlockSpec(memory_space=pltpu.VMEM)
    dma = pltpu.SemaphoreType.DMA
    whole, factors = pl.pallas_call(
        gather_kernel,
        out_shape=(
            pltpu.VMEM((KINDS, n * rows, columns), bf16),
            pltpu.VMEM((KINDS * n_col, LANES), f32),
        ),
        in_specs=[anywhere] * 10,
        out_specs=(local, local),
        scratch_shapes=[
            pltpu.VMEM((9, rows, columns), f32),
            pltpu.VMEM((KINDS, rows, columns), f32),
            pltpu.VMEM((1, rows), f32),
            pltpu.VMEM((rows, rows), f32),
            pltpu.VMEM((KINDS * n_col, LANES), f32),
            pltpu.VMEM((SIDE * SIDE, KINDS * n_col, LANES), f32),
            pltpu.VMEM((KINDS * n_col, LANES), f32),
            pltpu.VMEM((KINDS * n_col, LANES), f32),
            dma((10,)),
            dma((SIDE * SIDE,)),
            dma((SIDE * SIDE,)),
            dma,
            dma,
            dma((N_LINK,)),
            dma((N_LINK,)),
            dma((N_PAIR,)),
            dma((N_PAIR,)),
        ],
        compiler_params=pltpu.CompilerParams(
            collective_id=0, has_side_effects=True, vmem_limit_bytes=36 * 2**20
        ),
        name="gather",
    )(*weights, gain.reshape(1, rows))
    tile = jax.ShapeDtypeStruct((n_col, LANES), f32)
    matrix = jax.ShapeDtypeStruct((n * rows, columns), bf16)
    q, k, v, tq, tk, tv = pl.pallas_call(
        store_kernel,
        out_shape=(matrix, matrix, matrix, tile, tile, tile),
        in_specs=[local, local],
        out_specs=(anywhere,) * 6,
        scratch_shapes=[dma((24,)), dma((3,))],
        compiler_params=pltpu.CompilerParams(vmem_limit_bytes=32 * 2**20),
        name="store",
    )(whole, factors)
    return (q, k, v, tq.reshape(-1), tk.reshape(-1), tv.reshape(-1))


def solution(mesh):
    return jax.shard_map(
        on_device,
        mesh=mesh,
        in_specs=(P("fsdp", "model"),) * 9 + (P("fsdp"),),
        out_specs=(P(None, "model"),) * 3 + (P("model"),) * 3,
        check_vma=False,
    )
```

```python
import jax
import jax.numpy as jnp
from jax import lax
from jax.experimental import pallas as pl
from jax.experimental.pallas import tpu as pltpu
from jax.sharding import PartitionSpec as P

MESH = pl.DeviceIdType.MESH
D_MODEL = 4096
learn_rate = 0.2
hold_rate = 0.9

KINDS = 3
SIDE = 4
LANES = 128
QUARTER = 4


def arrivals():
    names = []
    for sign in (-1, 1):
        for half in (0, 1):
            names.append(("near", sign, half))
    for half in (0, 1):
        names.append(("far", 0, half))
    for first in (0, -1, 1, 2):
        for sign in (-1, 1):
            for half in (0, 1):
                names.append(("near2", first, sign, half))
        for half in (0, 1):
            names.append(("far2", first, 0, half))
    return names


NAMES = arrivals()
INDEX = {(color, name): color * len(NAMES) + k for color in (0, 1) for k, name in enumerate(NAMES)}
N_LINK = 2 * len(NAMES)
OWN = {(color, half): N_LINK + 2 * color + half for color in (0, 1) for half in (0, 1)}
N_PAIR = N_LINK + 4


def gather_kernel(
    wq, fq, sq, wk, fk, sk, wv, fv, sv, gain_ref,
    out, factor_ref,
    staged, gained, gain_row, gain_full, sums, every, mine, other,
    in_sem, sum_send, sum_recv, pair_send, pair_recv, link_send, link_recv, d2d_send, d2d_recv,
):
    me = lax.axis_index("fsdp")
    core = lax.rem(me, 2)
    chip = me // 2
    x = lax.rem(chip, SIDE)
    y = chip // SIDE
    rows = gained.shape[1]
    columns = gained.shape[2]
    n_col = columns // LANES
    piece = rows // QUARTER

    def device(dy, dx):
        return (lax.rem(y + dy + SIDE, SIDE) * SIDE + lax.rem(x + dx + SIDE, SIDE)) * 2 + core

    partner = chip * 2 + 1 - core

    loads = []
    for k, ref in enumerate((wq, fq, sq, wk, fk, sk, wv, fv, sv)):
        loads.append(pltpu.make_async_copy(ref, staged.at[k], in_sem.at[k]))
    loads.append(pltpu.make_async_copy(gain_ref, gain_row, in_sem.at[9]))
    loads[9].start()
    for k in range(9):
        loads[k].start()

    barrier = pltpu.get_barrier_semaphore()
    pl.semaphore_signal(barrier, inc=1, device_id={"fsdp": partner}, device_id_type=MESH)
    for k in range(1, SIDE * SIDE):
        pl.semaphore_signal(
            barrier, inc=1, device_id={"fsdp": device(k // SIDE, k % SIDE)}, device_id_type=MESH
        )

    loads[9].wait()
    gain_full[...] = jnp.broadcast_to(gain_row[...], (rows, rows)).T
    for m in range(KINDS):
        for k in range(3):
            loads[3 * m + k].wait()
        for j in range(n_col):
            at = slice(j * LANES, (j + 1) * LANES)
            hold = hold_rate * staged[3 * m + 1, :, at] + staged[3 * m + 2, :, at]
            latest = staged[3 * m, :, at] - learn_rate * hold
            value = latest * gain_full[...]
            gained[m, :, at] = value
            sums[m * n_col + j : m * n_col + j + 1, :] = jnp.sum(jnp.abs(value), axis=0, keepdims=True)

    pl.semaphore_wait(barrier, SIDE * SIDE)

    def sum_copy(k):
        return pltpu.make_async_remote_copy(
            src_ref=sums,
            dst_ref=every.at[chip],
            send_sem=sum_send.at[k],
            recv_sem=sum_recv.at[k],
            device_id={"fsdp": device(k // SIDE, k % SIDE)},
            device_id_type=MESH,
        )

    for k in (10, 11, 9, 14, 6, 2, 8, 5, 7, 13, 15, 1, 3, 4, 12):
        sum_copy(k).start()
    every[chip] = sums[...]
    for k in range(1, SIDE * SIDE):
        sum_copy(k).wait_recv()
    total = every[0]
    for k in range(1, SIDE * SIDE):
        total = total + every[k]
    mine[...] = total
    pair = pltpu.make_async_remote_copy(
        src_ref=mine,
        dst_ref=other,
        send_sem=pair_send,
        recv_sem=pair_recv,
        device_id={"fsdp": partner},
        device_id_type=MESH,
    )
    pair.start()
    pair.wait_recv()
    factor_ref[...] = (mine[...] + other[...]) / D_MODEL
    mine_recip = 1.0 / factor_ref[...]

    def block_start(color, first, second):
        dy, dx = (second, first) if color == 0 else (first, second)
        return device(dy, dx) * rows

    def place(color, first, second, half):
        at = pl.multiple_of(block_start(color, first, second) + (2 * color + half) * piece, piece)
        return out.at[:, pl.ds(at, piece), :]

    def neighbour(color, stage, sign):
        along_x = (color == 0) == (stage == 1)
        return device(0, sign) if along_x else device(sign, 0)

    def where(color, name):
        if name[0] == "near":
            return name[1], 0
        if name[0] == "far":
            return 2, 0
        if name[0] == "near2":
            return name[1], name[2]
        return name[1], 2

    sent = []

    def link(color, name, first, second, target):
        half = name[-1]
        k = INDEX[(color, name)]
        ref = place(color, first, second, half)
        return pltpu.make_async_remote_copy(
            src_ref=ref,
            dst_ref=ref,
            send_sem=link_send.at[k],
            recv_sem=link_recv.at[k],
            device_id={"fsdp": target},
            device_id_type=MESH,
        )

    def send(color, name, first, second, stage, sign):
        copy = link(color, name, first, second, neighbour(color, stage, sign))
        copy.start()
        sent.append(copy)

    def to_partner(k, color, first, second, half):
        ref = place(color, first, second, half)
        copy = pltpu.make_async_remote_copy(
            src_ref=ref,
            dst_ref=ref,
            send_sem=d2d_send.at[k],
            recv_sem=d2d_recv.at[k],
            device_id={"fsdp": partner},
            device_id_type=MESH,
        )
        copy.start()
        sent.append(copy)

    def arrived(color, name):
        first, second = where(color, name)
        link(color, name, first, second, me).wait_recv()
        half = name[-1]
        kind = name[0]
        if kind == "near":
            sign = name[1]
            if (sign, half) in ((-1, 0), (1, 1)):
                send(color, ("far", 0, half), first, second, 1, -sign)
        if kind in ("near", "far"):
            for to in (1, -1):
                send(color, ("near2", first, -to, half), first, second, 2, to)
        if kind == "near2":
            sign = name[2]
            if (sign, half) in ((-1, 0), (1, 1)):
                send(color, ("far2", first, 0, half), first, second, 2, -sign)
        to_partner(INDEX[(color, name)], color, first, second, half)

    order = ((0, 0), (1, 0), (0, 1), (1, 1))
    for color, half in order:
        low = (2 * color + half) * piece
        at = pl.multiple_of(me * rows + low, piece)
        for m in range(KINDS):
            for j in range(n_col):
                cols = slice(j * LANES, (j + 1) * LANES)
                row = m * n_col + j
                out[m, pl.ds(at, piece), cols] = (
                    gained[m, low : low + piece, cols] * mine_recip[row : row + 1, :]
                ).astype(out.dtype)
    for color in (0, 1):
        for to in (1, -1):
            for half in ((0, 1) if to == 1 else (1, 0)):
                send(color, ("near", -to, half), 0, 0, 1, to)
    for color in (0, 1):
        for to in (1, -1):
            for half in ((0, 1) if to == 1 else (1, 0)):
                send(color, ("near2", 0, -to, half), 0, 0, 2, to)
    for color, half in order:
        to_partner(OWN[(color, half)], color, 0, 0, half)

    both = (0, 1)
    for name in (("near", -1, 0), ("near", 1, 1), ("near", -1, 1), ("near", 1, 0)):
        for color in both:
            arrived(color, name)
    for name in (("near2", 0, -1, 0), ("near2", 0, 1, 1), ("near2", 0, -1, 1), ("near2", 0, 1, 0)):
        for color in both:
            arrived(color, name)
    for name in (("far", 0, 0), ("far", 0, 1)):
        for color in both:
            arrived(color, name)
    for first in (-1, 1, 2):
        for half in ((0, 1) if first != 1 else (1, 0)):
            for sign in (-1, 1):
                for color in both:
                    arrived(color, ("near2", first, sign, half))
        if first == -1:
            for half in (0, 1):
                for color in both:
                    arrived(color, ("far2", 0, 0, half))
    for first in (-1, 1, 2):
        for half in (0, 1):
            for color in both:
                arrived(color, ("far2", first, 0, half))

    def from_partner(k, color, first, second, half):
        dy, dx = (second, first) if color == 0 else (first, second)
        at = (device(dy, dx) + 1 - 2 * core) * rows + (2 * color + half) * piece
        ref = out.at[:, pl.ds(pl.multiple_of(at, piece), piece), :]
        pltpu.make_async_remote_copy(
            src_ref=ref,
            dst_ref=ref,
            send_sem=d2d_send.at[k],
            recv_sem=d2d_recv.at[k],
            device_id={"fsdp": partner},
            device_id_type=MESH,
        ).wait_recv()

    for color in both:
        for half in (0, 1):
            from_partner(OWN[(color, half)], color, 0, 0, half)
        for name in NAMES:
            from_partner(INDEX[(color, name)], color, *where(color, name), name[-1])
    for copy in sent:
        copy.wait_send()
    for k in range(1, SIDE * SIDE):
        sum_copy(k).wait_send()
    pair.wait_send()


def store_kernel(whole, factors, oq, ok, ov, tq, tk, tv, sem, small):
    n_row = oq.shape[0]
    parts = 8
    step = n_row // parts
    copies = []
    for m, ref in enumerate((oq, ok, ov)):
        for k in range(parts):
            copies.append(
                pltpu.make_async_copy(
                    whole.at[m, k * step : (k + 1) * step, :],
                    ref.at[k * step : (k + 1) * step, :],
                    sem.at[m * parts + k],
                )
            )
    n_col = tq.shape[0]
    for m, ref in enumerate((tq, tk, tv)):
        copies.append(
            pltpu.make_async_copy(factors.at[m * n_col : (m + 1) * n_col, :], ref, small.at[m])
        )
    for copy in copies:
        copy.start()
    for copy in copies:
        copy.wait()


def on_device(*args):
    weights, gain = args[:9], args[9]
    rows, columns = weights[0].shape
    n_col = columns // LANES
    n = lax.axis_size("fsdp")
    f32, bf16 = jnp.float32, jnp.bfloat16
    anywhere = pl.BlockSpec(memory_space=pl.ANY)
    local = pl.BlockSpec(memory_space=pltpu.VMEM)
    dma = pltpu.SemaphoreType.DMA
    whole, factors = pl.pallas_call(
        gather_kernel,
        out_shape=(
            pltpu.VMEM((KINDS, n * rows, columns), bf16),
            pltpu.VMEM((KINDS * n_col, LANES), f32),
        ),
        in_specs=[anywhere] * 10,
        out_specs=(local, local),
        scratch_shapes=[
            pltpu.VMEM((9, rows, columns), f32),
            pltpu.VMEM((KINDS, rows, columns), f32),
            pltpu.VMEM((1, rows), f32),
            pltpu.VMEM((rows, rows), f32),
            pltpu.VMEM((KINDS * n_col, LANES), f32),
            pltpu.VMEM((SIDE * SIDE, KINDS * n_col, LANES), f32),
            pltpu.VMEM((KINDS * n_col, LANES), f32),
            pltpu.VMEM((KINDS * n_col, LANES), f32),
            dma((10,)),
            dma((SIDE * SIDE,)),
            dma((SIDE * SIDE,)),
            dma,
            dma,
            dma((N_LINK,)),
            dma((N_LINK,)),
            dma((N_PAIR,)),
            dma((N_PAIR,)),
        ],
        compiler_params=pltpu.CompilerParams(
            collective_id=0, has_side_effects=True, vmem_limit_bytes=36 * 2**20
        ),
        name="gather",
    )(*weights, gain.reshape(1, rows))
    tile = jax.ShapeDtypeStruct((n_col, LANES), f32)
    matrix = jax.ShapeDtypeStruct((n * rows, columns), bf16)
    q, k, v, tq, tk, tv = pl.pallas_call(
        store_kernel,
        out_shape=(matrix, matrix, matrix, tile, tile, tile),
        in_specs=[local, local],
        out_specs=(anywhere,) * 6,
        scratch_shapes=[dma((24,)), dma((3,))],
        compiler_params=pltpu.CompilerParams(vmem_limit_bytes=4 * 2**20),
        name="store",
    )(
        pltpu.with_memory_space_constraint(whole, pltpu.VMEM),
        pltpu.with_memory_space_constraint(factors, pltpu.VMEM),
    )
    return (q, k, v, tq.reshape(-1), tk.reshape(-1), tv.reshape(-1))


def solution(mesh):
    return jax.shard_map(
        on_device,
        mesh=mesh,
        in_specs=(P("fsdp", "model"),) * 9 + (P("fsdp"),),
        out_specs=(P(None, "model"),) * 3 + (P("model"),) * 3,
        check_vma=False,
    )
```

```python
import jax
import jax.numpy as jnp
from jax import lax
from jax.experimental import pallas as pl
from jax.experimental.pallas import tpu as pltpu
from jax.sharding import PartitionSpec as P

MESH = pl.DeviceIdType.MESH
D_MODEL = 4096
learn_rate = 0.2
hold_rate = 0.9

KINDS = 3
SIDE = 4
LANES = 128
QUARTER = 4


LAST = 2
EARLY = 2


def arrivals():
    names = []
    for sign, half in ((-1, 1), (1, 0)):
        names.append(("near", sign, half))
    for half in (0, 1):
        names.append(("far", 0, half))
    for first in (0, -1, 1, 2):
        for sign in (-1, 1):
            for half in (0, 1):
                names.append(("near2", first, sign, half))
        for half in (0, 1):
            names.append(("far2", first, 0, half))
    table, at = {}, 0
    for color in (0, 1):
        for name in names:
            table[(color, name)] = at
            at += KINDS if name[:2] == ("far2", LAST) else 1
    return table, at, 2 * len(names)


INDEX, N_SEM, N_LINK = arrivals()
N_PAIR = N_LINK + 8


def gather_kernel(
    wq, fq, sq, wk, fk, sk, wv, fv, sv, gain_ref,
    out, factor_ref,
    staged, gained, early, gain_row, gain_full, sums, row_sums, every,
    in_sem, sum_send, row_recv, column_recv, early_send, early_recv, all_send, link_recv, d2d_recv,
):
    me = lax.axis_index("fsdp")
    core = lax.rem(me, 2)
    chip = me // 2
    x = lax.rem(chip, SIDE)
    y = chip // SIDE
    rows = gained.shape[1]
    columns = gained.shape[2]
    n_col = columns // LANES
    piece = rows // QUARTER

    def device(dy, dx, on=core):
        return (lax.rem(y + dy + SIDE, SIDE) * SIDE + lax.rem(x + dx + SIDE, SIDE)) * 2 + on

    partner = device(0, 0, 1 - core)
    row_peers = [partner] + [device(0, dx, on) for dx in (2, 1, 3) for on in (core, 1 - core)]
    column_peers = [device(dy, 0) for dy in (2, 1, 3)]

    barrier = pltpu.get_barrier_semaphore()
    for peer in column_peers + row_peers:
        pl.semaphore_signal(barrier, inc=1, device_id={"fsdp": peer}, device_id_type=MESH)

    weights = (wq, fq, sq, wk, fk, sk, wv, fv, sv)
    gain_load = pltpu.make_async_copy(gain_ref, gain_row, in_sem.at[KINDS])
    gain_load.start()
    for k, ref in enumerate(weights):
        pltpu.make_async_copy(ref, staged.at[k], in_sem.at[k // 3]).start()

    gain_load.wait()
    gain_full[...] = jnp.broadcast_to(gain_row[...], (rows, rows)).T
    for m in range(KINDS):
        all_three = staged.at[3 * m : 3 * m + 3]
        pltpu.make_async_copy(all_three, all_three, in_sem.at[m]).wait()
        for j in range(n_col):
            at = slice(j * LANES, (j + 1) * LANES)
            hold = hold_rate * staged[3 * m + 1, :, at] + staged[3 * m + 2, :, at]
            latest = staged[3 * m, :, at] - learn_rate * hold
            value = latest * gain_full[...]
            gained[m, :, at] = value
            sums[m * n_col + j : m * n_col + j + 1, :] = jnp.sum(jnp.abs(value), axis=0, keepdims=True)

    pl.semaphore_wait(barrier, len(row_peers) + len(column_peers))

    def neighbour(color, stage, sign):
        along_x = (color == 0) == (stage == 1)
        return device(0, sign) if along_x else device(sign, 0)

    part = piece // EARLY

    def early_copy(color, side, k):
        low = (2 * color + side) * piece + k * part
        return pltpu.make_async_remote_copy(
            src_ref=gained.at[:, low : low + part, :],
            dst_ref=early.at[color, side, k],
            send_sem=early_send,
            recv_sem=early_recv.at[(2 * color + side) * EARLY + k],
            device_id={"fsdp": neighbour(color, 1, 1 - 2 * side)},
            device_id_type=MESH,
        )

    n_row = 2 * SIDE

    def sum_copy(source, slot, recv_sem, target):
        return pltpu.make_async_remote_copy(
            src_ref=source,
            dst_ref=every.at[slot],
            send_sem=sum_send,
            recv_sem=recv_sem,
            device_id={"fsdp": target},
            device_id_type=MESH,
        )

    def wait_all(ref, sem):
        pltpu.make_async_copy(ref, ref, sem).wait()

    for peer in row_peers:
        sum_copy(sums, 2 * x + core, row_recv, peer).start()
    early_copy(1, 0, 0).start()
    early_copy(1, 1, 0).start()
    early_copy(0, 0, 0).start()
    early_copy(0, 1, 0).start()
    every[2 * x + core] = sums[...]
    wait_all(every.at[0 : n_row - 1], row_recv)
    total = every[0]
    for k in range(1, n_row):
        total = total + every[k]
    row_sums[...] = total
    for peer in column_peers:
        sum_copy(row_sums, n_row + y, column_recv, peer).start()
    early_copy(0, 0, 1).start()
    early_copy(0, 1, 1).start()
    early_copy(1, 0, 1).start()
    early_copy(1, 1, 1).start()
    every[n_row + y] = total
    wait_all(every.at[n_row : n_row + SIDE - 1], column_recv)
    total = every[n_row]
    for k in range(1, SIDE):
        total = total + every[n_row + k]
    factor_ref[...] = total / D_MODEL
    recip = 1.0 / factor_ref[...]

    def block_start(color, first, second):
        dy, dx = (second, first) if color == 0 else (first, second)
        return device(dy, dx) * rows

    def place(color, first, second, half):
        at = pl.multiple_of(block_start(color, first, second) + (2 * color + half) * piece, piece)
        return out.at[:, pl.ds(at, piece), :]

    def where(color, name):
        if name[0] == "near":
            return name[1], 0
        if name[0] == "far":
            return 2, 0
        if name[0] == "near2":
            return name[1], name[2]
        return name[1], 2

    def groups(name):
        if name[:2] == ("far2", LAST):
            return [(m, m + 1) for m in range(KINDS)]
        return [(0, KINDS)]

    def link(color, name, first, second, target, group):
        low, high = group
        ref = place(color, first, second, name[-1]).at[low:high]
        return pltpu.make_async_remote_copy(
            src_ref=ref,
            dst_ref=ref,
            send_sem=all_send,
            recv_sem=link_recv.at[INDEX[(color, name)] + low],
            device_id={"fsdp": target},
            device_id_type=MESH,
        )

    def send(color, name, first, second, stage, sign):
        for group in groups(name):
            link(color, name, first, second, neighbour(color, stage, sign), group).start()

    def to_partner(color, first, second, half, group=(0, KINDS)):
        ref = place(color, first, second, half).at[group[0] : group[1]]
        pltpu.make_async_remote_copy(
            src_ref=ref,
            dst_ref=ref,
            send_sem=all_send,
            recv_sem=d2d_recv,
            device_id={"fsdp": partner},
            device_id_type=MESH,
        ).start()

    def arrived(color, name, group=(0, KINDS)):
        first, second = where(color, name)
        link(color, name, first, second, partner, group).wait_recv()
        half = name[-1]
        if name[0] in ("near", "far"):
            first_axis_done(color, first, half)
        if name[0] == "near2" and (name[2], half) in ((-1, 0), (1, 1)):
            send(color, ("far2", first, 0, half), first, second, 2, -name[2])
        to_partner(color, first, second, half, group)

    def first_axis_done(color, first, half):
        for to in (1, -1) if half == 0 else (-1, 1):
            send(color, ("near2", first, -to, half), first, 0, 2, to)

    def scaled(color, first, half, source, low, count):
        start = block_start(color, first, 0) + (2 * color + half) * piece + low
        at = pl.multiple_of(start, count)
        for m in range(KINDS):
            for j in range(n_col):
                cols = slice(j * LANES, (j + 1) * LANES)
                row = m * n_col + j
                out[m, pl.ds(at, count), cols] = (
                    source(m, cols) * recip[row : row + 1, :]
                ).astype(out.dtype)

    both = (0, 1)
    halves = (0, 1)
    for half in halves:
        for color in both:
            low = (2 * color + half) * piece
            scaled(color, 0, half, lambda m, cols: gained[m, low : low + piece, cols], 0, piece)
    for half in halves:
        for color in both:
            to = 1 if half == 1 else -1
            send(color, ("near", -to, half), 0, 0, 1, to)
    for color in both:
        for side in halves:
            first = 2 * side - 1
            for k in range(EARLY):
                early_copy(color, side, k).wait_recv()
                scaled(color, first, side, lambda m, cols: early[color, side, k, m, :, cols], k * part, part)
    for half in halves:
        for color in both:
            first_axis_done(color, 0, half)
    for color in both:
        for side in halves:
            first = 2 * side - 1
            send(color, ("far", 0, side), first, 0, 1, -first)
    for color in both:
        for side in halves:
            first_axis_done(color, 2 * side - 1, side)
    for color in both:
        for half in halves:
            to_partner(color, 0, 0, half)
            to_partner(color, 2 * half - 1, 0, half)

    for name in (("near", -1, 1), ("near", 1, 0)):
        for color in both:
            arrived(color, name)
    for name in (("near2", 0, -1, 0), ("near2", 0, 1, 1), ("near2", 0, -1, 1), ("near2", 0, 1, 0)):
        for color in both:
            arrived(color, name)
    for name in (("far", 0, 0), ("far", 0, 1)):
        for color in both:
            arrived(color, name)
    for first in (-1, 1, 2):
        for half in ((0, 1) if first != 1 else (1, 0)):
            for sign in (-1, 1):
                for color in both:
                    arrived(color, ("near2", first, sign, half))
        if first == -1:
            for half in halves:
                for color in both:
                    arrived(color, ("far2", 0, 0, half))
    for first in (-1, 1, LAST):
        name = ("far2", first, 0)
        for group in groups(name):
            for half in halves:
                for color in both:
                    arrived(color, (*name, half), group)

    wait_all(out.at[:, 0 : N_PAIR * piece, :], d2d_recv)
    wait_all(out.at[:, 0 : (N_LINK + N_PAIR) * piece, :], all_send)
    wait_all(early, early_send)
    wait_all(every.at[0 : len(row_peers) + len(column_peers)], sum_send)


def store_kernel(whole, factors, oq, ok, ov, tq, tk, tv, sem, small):
    n_row = oq.shape[0]
    parts = 8
    step = n_row // parts
    copies = []
    for m, ref in enumerate((oq, ok, ov)):
        for k in range(parts):
            copies.append(
                pltpu.make_async_copy(
                    whole.at[m, k * step : (k + 1) * step, :],
                    ref.at[k * step : (k + 1) * step, :],
                    sem,
                )
            )
    n_col = tq.shape[0]
    for m, ref in enumerate((tq, tk, tv)):
        copies.append(
            pltpu.make_async_copy(factors.at[m * n_col : (m + 1) * n_col, :], ref, small)
        )
    for copy in copies:
        copy.start()
    pltpu.make_async_copy(whole, whole, sem).wait()
    pltpu.make_async_copy(factors, factors, small).wait()


def on_device(*args):
    weights, gain = args[:9], args[9]
    rows, columns = weights[0].shape
    n_col = columns // LANES
    n = lax.axis_size("fsdp")
    f32, bf16 = jnp.float32, jnp.bfloat16
    anywhere = pl.BlockSpec(memory_space=pl.ANY)
    local = pl.BlockSpec(memory_space=pltpu.VMEM)
    dma = pltpu.SemaphoreType.DMA
    whole, factors = pl.pallas_call(
        gather_kernel,
        out_shape=(
            pltpu.VMEM((KINDS, n * rows, columns), bf16),
            pltpu.VMEM((KINDS * n_col, LANES), f32),
        ),
        in_specs=[anywhere] * 10,
        out_specs=(local, local),
        scratch_shapes=[
            pltpu.VMEM((9, rows, columns), f32),
            pltpu.VMEM((KINDS, rows, columns), f32),
            pltpu.VMEM((2, 2, EARLY, KINDS, rows // QUARTER // EARLY, columns), f32),
            pltpu.VMEM((1, rows), f32),
            pltpu.VMEM((rows, rows), f32),
            pltpu.VMEM((KINDS * n_col, LANES), f32),
            pltpu.VMEM((KINDS * n_col, LANES), f32),
            pltpu.VMEM((3 * SIDE, KINDS * n_col, LANES), f32),
            dma((KINDS + 1,)),
            dma,
            dma,
            dma,
            dma,
            dma((4 * EARLY,)),
            dma,
            dma((N_SEM,)),
            dma,
        ],
        compiler_params=pltpu.CompilerParams(
            collective_id=0, has_side_effects=True, vmem_limit_bytes=36 * 2**20
        ),
        name="gather",
    )(*weights, gain.reshape(1, rows))
    tile = jax.ShapeDtypeStruct((n_col, LANES), f32)
    matrix = jax.ShapeDtypeStruct((n * rows, columns), bf16)
    q, k, v, tq, tk, tv = pl.pallas_call(
        store_kernel,
        out_shape=(matrix, matrix, matrix, tile, tile, tile),
        in_specs=[local, local],
        out_specs=(anywhere,) * 6,
        scratch_shapes=[dma, dma],
        compiler_params=pltpu.CompilerParams(vmem_limit_bytes=4 * 2**20),
        name="store",
    )(
        pltpu.with_memory_space_constraint(whole, pltpu.VMEM),
        pltpu.with_memory_space_constraint(factors, pltpu.VMEM),
    )
    return (q, k, v, tq.reshape(-1), tk.reshape(-1), tv.reshape(-1))


def solution(mesh):
    return jax.shard_map(
        on_device,
        mesh=mesh,
        in_specs=(P("fsdp", "model"),) * 9 + (P("fsdp"),),
        out_specs=(P(None, "model"),) * 3 + (P("model"),) * 3,
        check_vma=False,
    )
```

```python
import jax
import jax.numpy as jnp
from jax import lax
from jax.experimental import pallas as pl
from jax.experimental.pallas import tpu as pltpu
from jax.sharding import PartitionSpec as P

MESH = pl.DeviceIdType.MESH
D_MODEL = 4096
learn_rate = 0.2
hold_rate = 0.9

KINDS = 3
SIDE = 4
LANES = 128
QUARTER = 4


LAST = 2
EARLY = ((0, 16), (16, 8))


def arrivals():
    names = []
    for sign in (-1, 1):
        for half in (0, 1):
            names.append(("near", sign, half))
    for half in (0, 1):
        names.append(("far", 0, half))
    for first in (0, -1, 1, 2):
        for sign in (-1, 1):
            for half in (0, 1):
                names.append(("near2", first, sign, half))
        for half in (0, 1):
            names.append(("far2", first, 0, half))
    table, at = {}, 0
    for color in (0, 1):
        for name in names:
            table[(color, name)] = at
            at += KINDS if name[:2] == ("far2", LAST) else 1
    return table, at, 2 * len(names)


INDEX, N_SEM, N_LINK = arrivals()
EARLY_NAMES = (("near", -1, 0), ("near", 1, 1))
N_PAIR = N_LINK + 4


def gather_kernel(
    wq, fq, sq, wk, fk, sk, wv, fv, sv, gain_ref,
    out, factor_ref,
    staged, gained, early, gain_row, gain_full, sums, row_sums, every,
    in_sem, sum_send, row_recv, column_recv, early_send, early_recv, all_send, link_recv, d2d_recv,
):
    me = lax.axis_index("fsdp")
    core = lax.rem(me, 2)
    chip = me // 2
    x = lax.rem(chip, SIDE)
    y = chip // SIDE
    rows = gained.shape[1]
    columns = gained.shape[2]
    n_col = columns // LANES
    piece = rows // QUARTER

    def device(dy, dx, on=core):
        return (lax.rem(y + dy + SIDE, SIDE) * SIDE + lax.rem(x + dx + SIDE, SIDE)) * 2 + on

    partner = device(0, 0, 1 - core)
    row_peers = [partner] + [device(0, dx, on) for dx in (2, 1, 3) for on in (core, 1 - core)]
    column_peers = [device(dy, 0) for dy in (2, 1, 3)]

    barrier = pltpu.get_barrier_semaphore()
    for peer in column_peers + row_peers:
        pl.semaphore_signal(barrier, inc=1, device_id={"fsdp": peer}, device_id_type=MESH)

    weights = (wq, fq, sq, wk, fk, sk, wv, fv, sv)
    gain_load = pltpu.make_async_copy(gain_ref, gain_row, in_sem.at[KINDS])
    gain_load.start()
    for k, ref in enumerate(weights):
        pltpu.make_async_copy(ref, staged.at[k], in_sem.at[k // 3]).start()

    gain_load.wait()
    gain_full[...] = jnp.broadcast_to(gain_row[...], (rows, rows)).T
    for m in range(KINDS):
        all_three = staged.at[3 * m : 3 * m + 3]
        pltpu.make_async_copy(all_three, all_three, in_sem.at[m]).wait()
        for j in range(n_col):
            at = slice(j * LANES, (j + 1) * LANES)
            hold = hold_rate * staged[3 * m + 1, :, at] + staged[3 * m + 2, :, at]
            latest = staged[3 * m, :, at] - learn_rate * hold
            value = latest * gain_full[...]
            gained[m, :, at] = value
            sums[m * n_col + j : m * n_col + j + 1, :] = jnp.sum(jnp.abs(value), axis=0, keepdims=True)

    pl.semaphore_wait(barrier, len(row_peers) + len(column_peers))

    def neighbour(color, stage, sign):
        along_x = (color == 0) == (stage == 1)
        return device(0, sign) if along_x else device(sign, 0)

    part = sum(count for _, count in EARLY)

    def early_copy(color, side, k):
        start, count = EARLY[k]
        low = (2 * color + side) * piece + start
        return pltpu.make_async_remote_copy(
            src_ref=gained.at[:, low : low + count, :],
            dst_ref=early.at[color, side, :, start : start + count, :],
            send_sem=early_send,
            recv_sem=early_recv.at[(2 * color + side) * len(EARLY) + k],
            device_id={"fsdp": neighbour(color, 1, 1 - 2 * side)},
            device_id_type=MESH,
        )

    n_row = 2 * SIDE

    def sum_copy(source, slot, recv_sem, target):
        return pltpu.make_async_remote_copy(
            src_ref=source,
            dst_ref=every.at[slot],
            send_sem=sum_send,
            recv_sem=recv_sem,
            device_id={"fsdp": target},
            device_id_type=MESH,
        )

    def wait_all(ref, sem):
        pltpu.make_async_copy(ref, ref, sem).wait()

    for peer in row_peers:
        sum_copy(sums, 2 * x + core, row_recv, peer).start()
    for color in (1, 0):
        for side in (0, 1):
            early_copy(color, side, 0).start()
    every[2 * x + core] = sums[...]
    wait_all(every.at[0 : n_row - 1], row_recv)
    total = every[0]
    for k in range(1, n_row):
        total = total + every[k]
    row_sums[...] = total
    for peer in column_peers:
        sum_copy(row_sums, n_row + y, column_recv, peer).start()
    for k in range(1, len(EARLY)):
        for color in (1, 0):
            for side in (0, 1):
                early_copy(color, side, k).start()
    every[n_row + y] = total
    wait_all(every.at[n_row : n_row + SIDE - 1], column_recv)
    total = every[n_row]
    for k in range(1, SIDE):
        total = total + every[n_row + k]
    factor_ref[...] = total / D_MODEL
    recip = 1.0 / factor_ref[...]

    def block_start(color, first, second):
        dy, dx = (second, first) if color == 0 else (first, second)
        return device(dy, dx) * rows

    def place(color, first, second, half, skip=0):
        at = block_start(color, first, second) + (2 * color + half) * piece + skip
        return out.at[:, pl.ds(pl.multiple_of(at, 8 if skip else piece), piece - skip), :]

    def where(color, name):
        if name[0] == "near":
            return name[1], 0
        if name[0] == "far":
            return 2, 0
        if name[0] == "near2":
            return name[1], name[2]
        return name[1], 2

    def groups(name):
        if name[:2] == ("far2", LAST):
            return [(m, m + 1) for m in range(KINDS)]
        return [(0, KINDS)]

    def link(color, name, first, second, target, group):
        low, high = group
        skip = part if name in EARLY_NAMES else 0
        ref = place(color, first, second, name[-1], skip).at[low:high]
        return pltpu.make_async_remote_copy(
            src_ref=ref,
            dst_ref=ref,
            send_sem=all_send,
            recv_sem=link_recv.at[INDEX[(color, name)] + low],
            device_id={"fsdp": target},
            device_id_type=MESH,
        )

    def send(color, name, first, second, stage, sign):
        for group in groups(name):
            link(color, name, first, second, neighbour(color, stage, sign), group).start()

    def to_partner(color, first, second, half, group=(0, KINDS)):
        ref = place(color, first, second, half).at[group[0] : group[1]]
        pltpu.make_async_remote_copy(
            src_ref=ref,
            dst_ref=ref,
            send_sem=all_send,
            recv_sem=d2d_recv,
            device_id={"fsdp": partner},
            device_id_type=MESH,
        ).start()

    def arrived(color, name, group=(0, KINDS)):
        first, second = where(color, name)
        link(color, name, first, second, partner, group).wait_recv()
        half = name[-1]
        if name in EARLY_NAMES:
            send(color, ("far", 0, half), first, 0, 1, -first)
        if name[0] in ("near", "far"):
            first_axis_done(color, first, half)
        if name[0] == "near2" and (name[2], half) in ((-1, 0), (1, 1)):
            send(color, ("far2", first, 0, half), first, second, 2, -name[2])
        to_partner(color, first, second, half, group)

    def first_axis_done(color, first, half):
        for to in (1, -1) if half == 0 else (-1, 1):
            send(color, ("near2", first, -to, half), first, 0, 2, to)

    def scaled(color, first, half, source, low, count):
        start = block_start(color, first, 0) + (2 * color + half) * piece + low
        at = pl.multiple_of(start, 8)
        for m in range(KINDS):
            for j in range(n_col):
                cols = slice(j * LANES, (j + 1) * LANES)
                row = m * n_col + j
                out[m, pl.ds(at, count), cols] = (
                    source(m, cols) * recip[row : row + 1, :]
                ).astype(out.dtype)

    both = (0, 1)
    halves = (0, 1)
    def own(half, color, low, count):
        base = (2 * color + half) * piece + low
        scaled(color, 0, half, lambda m, cols: gained[m, base : base + count, cols], low, count)

    for same in (True, False):
        for half in halves:
            for color in both:
                if same:
                    own(half, color, part, piece - part)
                else:
                    own(half, color, 0, part)
        for half in halves:
            for color in both:
                to = 1 if (half == 0) == same else -1
                send(color, ("near", -to, half), 0, 0, 1, to)
    for half in halves:
        for color in both:
            first_axis_done(color, 0, half)
    for color in both:
        for side in halves:
            for k, (start, count) in enumerate(EARLY):
                early_copy(color, side, k).wait_recv()
                rows_of = slice(start, start + count)
                scaled(
                    color, 2 * side - 1, side,
                    lambda m, cols: early[color, side, m, rows_of, cols], start, count,
                )
    for color in both:
        for half in halves:
            to_partner(color, 0, 0, half)

    for name in (*EARLY_NAMES, ("near", -1, 1), ("near", 1, 0)):
        for color in both:
            arrived(color, name)
    for name in (("near2", 0, -1, 0), ("near2", 0, 1, 1), ("near2", 0, -1, 1), ("near2", 0, 1, 0)):
        for color in both:
            arrived(color, name)
    for name in (("far", 0, 0), ("far", 0, 1)):
        for color in both:
            arrived(color, name)
    for first in (-1, 1, 2):
        for half in ((0, 1) if first != 1 else (1, 0)):
            for sign in (-1, 1):
                for color in both:
                    arrived(color, ("near2", first, sign, half))
        if first == -1:
            for half in halves:
                for color in both:
                    arrived(color, ("far2", 0, 0, half))
    for first in (-1, 1, LAST):
        name = ("far2", first, 0)
        for group in groups(name):
            for half in halves:
                for color in both:
                    arrived(color, (*name, half), group)

    wait_all(out.at[:, 0 : N_PAIR * piece, :], d2d_recv)
    wait_all(out.at[:, 0 : (N_LINK + N_PAIR) * piece - 4 * part, :], all_send)
    wait_all(early, early_send)
    wait_all(every.at[0 : len(row_peers) + len(column_peers)], sum_send)


def store_kernel(whole, factors, oq, ok, ov, tq, tk, tv, sem, small):
    n_row = oq.shape[0]
    parts = 8
    step = n_row // parts
    copies = []
    for m, ref in enumerate((oq, ok, ov)):
        for k in range(parts):
            copies.append(
                pltpu.make_async_copy(
                    whole.at[m, k * step : (k + 1) * step, :],
                    ref.at[k * step : (k + 1) * step, :],
                    sem,
                )
            )
    n_col = tq.shape[0]
    for m, ref in enumerate((tq, tk, tv)):
        copies.append(
            pltpu.make_async_copy(factors.at[m * n_col : (m + 1) * n_col, :], ref, small)
        )
    for copy in copies:
        copy.start()
    pltpu.make_async_copy(whole, whole, sem).wait()
    pltpu.make_async_copy(factors, factors, small).wait()


def on_device(*args):
    weights, gain = args[:9], args[9]
    rows, columns = weights[0].shape
    n_col = columns // LANES
    n = lax.axis_size("fsdp")
    f32, bf16 = jnp.float32, jnp.bfloat16
    anywhere = pl.BlockSpec(memory_space=pl.ANY)
    local = pl.BlockSpec(memory_space=pltpu.VMEM)
    dma = pltpu.SemaphoreType.DMA
    whole, factors = pl.pallas_call(
        gather_kernel,
        out_shape=(
            pltpu.VMEM((KINDS, n * rows, columns), bf16),
            pltpu.VMEM((KINDS * n_col, LANES), f32),
        ),
        in_specs=[anywhere] * 10,
        out_specs=(local, local),
        scratch_shapes=[
            pltpu.VMEM((9, rows, columns), f32),
            pltpu.VMEM((KINDS, rows, columns), f32),
            pltpu.VMEM((2, 2, KINDS, sum(count for _, count in EARLY), columns), f32),
            pltpu.VMEM((1, rows), f32),
            pltpu.VMEM((rows, rows), f32),
            pltpu.VMEM((KINDS * n_col, LANES), f32),
            pltpu.VMEM((KINDS * n_col, LANES), f32),
            pltpu.VMEM((3 * SIDE, KINDS * n_col, LANES), f32),
            dma((KINDS + 1,)),
            dma,
            dma,
            dma,
            dma,
            dma((4 * len(EARLY),)),
            dma,
            dma((N_SEM,)),
            dma,
        ],
        compiler_params=pltpu.CompilerParams(
            collective_id=0, has_side_effects=True, vmem_limit_bytes=36 * 2**20
        ),
        name="gather",
    )(*weights, gain.reshape(1, rows))
    tile = jax.ShapeDtypeStruct((n_col, LANES), f32)
    matrix = jax.ShapeDtypeStruct((n * rows, columns), bf16)
    q, k, v, tq, tk, tv = pl.pallas_call(
        store_kernel,
        out_shape=(matrix, matrix, matrix, tile, tile, tile),
        in_specs=[local, local],
        out_specs=(anywhere,) * 6,
        scratch_shapes=[dma, dma],
        compiler_params=pltpu.CompilerParams(vmem_limit_bytes=4 * 2**20),
        name="store",
    )(
        pltpu.with_memory_space_constraint(whole, pltpu.VMEM),
        pltpu.with_memory_space_constraint(factors, pltpu.VMEM),
    )
    return (q, k, v, tq.reshape(-1), tk.reshape(-1), tv.reshape(-1))


def solution(mesh):
    return jax.shard_map(
        on_device,
        mesh=mesh,
        in_specs=(P("fsdp", "model"),) * 9 + (P("fsdp"),),
        out_specs=(P(None, "model"),) * 3 + (P("model"),) * 3,
        check_vma=False,
    )
```

```python
import jax
import jax.numpy as jnp
from jax import lax
from jax.experimental import pallas as pl
from jax.experimental.pallas import tpu as pltpu
from jax.sharding import PartitionSpec as P

MESH = pl.DeviceIdType.MESH
D_MODEL = 4096
learn_rate = 0.2
hold_rate = 0.9

KINDS = 3
SIDE = 4
LANES = 128
QUARTER = 4


LAST = 2
EARLY = (((0, 8), (8, 16)), ((0, 8), (8, 16)))
EARLY_ROWS = 24
EARLY_NAMES = (("near", -1, 0), ("near", 1, 1))


def groups():
    taken = [EARLY_NAMES, (("near", -1, 1), ("near", 1, 0))]
    for first in (0, -1, 1, 2):
        if first == -1:
            taken.append((("far", 0, 0), ("far", 0, 1)))
        taken.append((("near2", first, -1, 0), ("near2", first, 1, 1)))
        taken.append((("near2", first, -1, 1), ("near2", first, 1, 0)))
        if first == 1:
            taken.append((("far2", 0, 0, 0), ("far2", 0, 0, 1)))
    for first in (-1, 1, LAST):
        taken.append((("far2", first, 0, 0), ("far2", first, 0, 1)))
    return taken


GROUPS = groups()
GROUP_OF = {name: k for k, names in enumerate(GROUPS) for name in names}
N_SEM = len(GROUPS) + KINDS - 1
N_LINK = 4 * len(GROUPS)
N_PAIR = N_LINK + 4


def gather_kernel(
    wq, fq, sq, wk, fk, sk, wv, fv, sv, gain_ref,
    out, factor_ref,
    staged, gained, early, gain_row, gain_full, sums, row_sums, every,
    in_sem, sum_send, row_recv, column_recv, early_send, early_recv, all_send, link_recv, d2d_recv,
):
    me = lax.axis_index("fsdp")
    core = lax.rem(me, 2)
    chip = me // 2
    x = lax.rem(chip, SIDE)
    y = chip // SIDE
    rows = gained.shape[1]
    columns = gained.shape[2]
    n_col = columns // LANES
    piece = rows // QUARTER

    def device(dy, dx, on=core):
        return (lax.rem(y + dy + SIDE, SIDE) * SIDE + lax.rem(x + dx + SIDE, SIDE)) * 2 + on

    partner = device(0, 0, 1 - core)
    row_peers = [device(0, dx, on) for dx in (2, 1, 3) for on in (0, 1)] + [partner]
    column_peers = [device(dy, 0, on) for dy in (2, 1, 3) for on in (0, 1)]

    def wait_all(ref, sem):
        pltpu.make_async_copy(ref, ref, sem).wait()

    weights = (wq, fq, sq, wk, fk, sk, wv, fv, sv)
    gain_load = pltpu.make_async_copy(gain_ref, gain_row, in_sem.at[KINDS])
    gain_load.start()
    for k, ref in enumerate(weights):
        pltpu.make_async_copy(ref, staged.at[k], in_sem.at[k // 3]).start()

    barrier = pltpu.get_barrier_semaphore()
    for peer in column_peers + row_peers:
        pl.semaphore_signal(barrier, inc=1, device_id={"fsdp": peer}, device_id_type=MESH)

    gain_load.wait()
    gain_full[...] = jnp.broadcast_to(gain_row[...], (rows, rows)).T
    for m in range(KINDS):
        all_three = staged.at[3 * m : 3 * m + 3]
        pltpu.make_async_copy(all_three, all_three, in_sem.at[m]).wait()
        for j in range(n_col):
            at = slice(j * LANES, (j + 1) * LANES)
            hold = hold_rate * staged[3 * m + 1, :, at] + staged[3 * m + 2, :, at]
            latest = staged[3 * m, :, at] - learn_rate * hold
            value = latest * gain_full[...]
            gained[m, :, at] = value
            sums[m * n_col + j : m * n_col + j + 1, :] = jnp.sum(jnp.abs(value), axis=0, keepdims=True)

    pl.semaphore_wait(barrier, len(row_peers) + len(column_peers))

    def neighbour(color, stage, sign):
        along_x = (color == 0) == (stage == 1)
        return device(0, sign) if along_x else device(sign, 0)

    part = EARLY_ROWS

    def early_copy(color, side, k):
        start, count = EARLY[color][k]
        low = (2 * color + side) * piece + start
        return pltpu.make_async_remote_copy(
            src_ref=gained.at[:, low : low + count, :],
            dst_ref=early.at[color, side, :, start : start + count, :],
            send_sem=early_send,
            recv_sem=early_recv.at[2 * color + k],
            device_id={"fsdp": neighbour(color, 1, 1 - 2 * side)},
            device_id_type=MESH,
        )

    def sum_copy(source, slot, recv_sem, target):
        return pltpu.make_async_remote_copy(
            src_ref=source,
            dst_ref=every.at[slot],
            send_sem=sum_send,
            recv_sem=recv_sem,
            device_id={"fsdp": target},
            device_id_type=MESH,
        )

    n_row = 2 * SIDE
    hub = 1
    for dx in (2, 1, 3):
        sum_copy(sums, 2 * x + core, row_recv, device(0, dx, hub)).start()

    @pl.when(core != hub)
    def _():
        sum_copy(sums, 2 * x + core, row_recv, partner).start()

    for color in (1, 0):
        for side in (0, 1):
            early_copy(color, side, 0).start()

    @pl.when(core == hub)
    def _():
        every[2 * x + core] = sums[...]
        wait_all(every.at[0 : n_row - 1], row_recv)
        total = every[0]
        for k in range(1, n_row):
            total = total + every[k]
        row_sums[...] = total
        for peer in [*column_peers, partner]:
            sum_copy(row_sums, n_row + y, column_recv, peer).start()
        every[n_row + y] = total

    for color in (0, 1):
        for side in (0, 1):
            early_copy(color, side, 1).start()

    @pl.when(core == hub)
    def _():
        wait_all(every.at[n_row : n_row + SIDE - 1], column_recv)

    @pl.when(core != hub)
    def _():
        wait_all(every.at[n_row : n_row + SIDE], column_recv)

    total = every[n_row]
    for k in range(1, SIDE):
        total = total + every[n_row + k]
    factor_ref[...] = total / D_MODEL
    recip = 1.0 / factor_ref[...]

    def block_start(color, first, second):
        dy, dx = (second, first) if color == 0 else (first, second)
        return device(dy, dx) * rows

    both = (0, 1)

    def place(color, first, second, half, skip=0):
        at = block_start(color, first, second) + (2 * color + half) * piece + skip
        return out.at[:, pl.ds(pl.multiple_of(at, 8 if skip else piece), piece - skip), :]

    def where(color, name):
        if name[0] == "near":
            return name[1], 0
        if name[0] == "far":
            return 2, 0
        if name[0] == "near2":
            return name[1], name[2]
        return name[1], 2

    def link(color, name, first, second, target, group):
        low, high = group
        skip = part if name in EARLY_NAMES else 0
        ref = place(color, first, second, name[-1], skip).at[low:high]
        return pltpu.make_async_remote_copy(
            src_ref=ref,
            dst_ref=ref,
            send_sem=all_send,
            recv_sem=link_recv.at[GROUP_OF[name] + (low if high - low < KINDS else 0)],
            device_id={"fsdp": target},
            device_id_type=MESH,
        )

    def send(color, name, first, second, stage, sign):
        whole = [(m, m + 1) for m in range(KINDS)] if name[:2] == ("far2", LAST) else [(0, KINDS)]
        for group in whole:
            link(color, name, first, second, neighbour(color, stage, sign), group).start()

    def to_partner(color, first, second, half, group=(0, KINDS)):
        ref = place(color, first, second, half).at[group[0] : group[1]]
        pltpu.make_async_remote_copy(
            src_ref=ref,
            dst_ref=ref,
            send_sem=all_send,
            recv_sem=d2d_recv,
            device_id={"fsdp": partner},
            device_id_type=MESH,
        ).start()

    def arrived(color, name, group):
        first, second = where(color, name)
        half = name[-1]
        if name in EARLY_NAMES:
            send(color, ("far", 0, half), first, 0, 1, -first)
        if name[0] == "near":
            for to in (1, -1) if half == 0 else (-1, 1):
                send(color, ("near2", first, -to, half), first, 0, 2, to)
        if name[0] == "near2" and (name[2], half) in ((-1, 0), (1, 1)):
            send(color, ("far2", first, 0, half), first, second, 2, -name[2])

    def both_halves(first):
        for at in (0, 1):
            for to in (1, -1):
                half = at if to == 1 else 1 - at
                for color in both:
                    send(color, ("near2", first, -to, half), first, 0, 2, to)

    def take(k, group=(0, KINDS)):
        low, high = group
        count = 4 * (piece - part if GROUPS[k] == EARLY_NAMES else piece)
        wait_all(out.at[low:high, 0:count, :], link_recv.at[k + (low if high - low < KINDS else 0)])
        for name in GROUPS[k]:
            for color in both:
                arrived(color, name, group)
        if GROUPS[k][0][0] == "far":
            both_halves(2)
        for name in GROUPS[k]:
            for color in both:
                to_partner(color, *where(color, name), name[-1], group)

    def scaled(color, first, half, source, low, count):
        start = block_start(color, first, 0) + (2 * color + half) * piece + low
        at = pl.multiple_of(start, 8)
        for m in range(KINDS):
            for j in range(n_col):
                cols = slice(j * LANES, (j + 1) * LANES)
                row = m * n_col + j
                out[m, pl.ds(at, count), cols] = (
                    source(m, cols) * recip[row : row + 1, :]
                ).astype(out.dtype)

    halves = (0, 1)
    def own(half, color, low, count):
        base = (2 * color + half) * piece + low
        scaled(color, 0, half, lambda m, cols: gained[m, base : base + count, cols], low, count)

    for same in (True, False):
        for half in halves:
            for color in both:
                if same:
                    own(half, color, part, piece - part)
                else:
                    own(half, color, 0, part)
        for half in halves:
            for color in both:
                to = 1 if (half == 0) == same else -1
                send(color, ("near", -to, half), 0, 0, 1, to)
    both_halves(0)
    for color in both:
        for k in range(2):
            start, count = EARLY[color][k]
            wait_all(early.at[color, :, :, start : start + count, :], early_recv.at[2 * color + k])
            for side in halves:
                rows_of = slice(start, start + count)
                scaled(
                    color, 2 * side - 1, side,
                    lambda m, cols: early[color, side, m, rows_of, cols], start, count,
                )
    for color in both:
        for half in halves:
            to_partner(color, 0, 0, half)

    for k in range(len(GROUPS) - 1):
        take(k)
    for m in range(KINDS):
        take(len(GROUPS) - 1, (m, m + 1))

    wait_all(out.at[:, 0 : N_PAIR * piece, :], d2d_recv)
    wait_all(out.at[:, 0 : (N_LINK + N_PAIR) * piece - 4 * part, :], all_send)
    wait_all(early, early_send)

    @pl.when(core == hub)
    def _():
        wait_all(every.at[0 : SIDE - 1 + len(column_peers) + 1], sum_send)

    @pl.when(core != hub)
    def _():
        wait_all(every.at[0:SIDE], sum_send)


def store_kernel(whole, factors, oq, ok, ov, tq, tk, tv, sem, small):
    n_row = oq.shape[0]
    parts = 8
    step = n_row // parts
    copies = []
    for m, ref in enumerate((oq, ok, ov)):
        for k in range(parts):
            copies.append(
                pltpu.make_async_copy(
                    whole.at[m, k * step : (k + 1) * step, :],
                    ref.at[k * step : (k + 1) * step, :],
                    sem,
                )
            )
    n_col = tq.shape[0]
    for m, ref in enumerate((tq, tk, tv)):
        copies.append(
            pltpu.make_async_copy(factors.at[m * n_col : (m + 1) * n_col, :], ref, small)
        )
    for copy in copies:
        copy.start()
    pltpu.make_async_copy(whole, whole, sem).wait()
    pltpu.make_async_copy(factors, factors, small).wait()


def on_device(*args):
    weights, gain = args[:9], args[9]
    rows, columns = weights[0].shape
    n_col = columns // LANES
    n = lax.axis_size("fsdp")
    f32, bf16 = jnp.float32, jnp.bfloat16
    anywhere = pl.BlockSpec(memory_space=pl.ANY)
    local = pl.BlockSpec(memory_space=pltpu.VMEM)
    dma = pltpu.SemaphoreType.DMA
    whole, factors = pl.pallas_call(
        gather_kernel,
        out_shape=(
            pltpu.VMEM((KINDS, n * rows, columns), bf16),
            pltpu.VMEM((KINDS * n_col, LANES), f32),
        ),
        in_specs=[anywhere] * 10,
        out_specs=(local, local),
        scratch_shapes=[
            pltpu.VMEM((9, rows, columns), f32),
            pltpu.VMEM((KINDS, rows, columns), f32),
            pltpu.VMEM((2, 2, KINDS, EARLY_ROWS, columns), f32),
            pltpu.VMEM((1, rows), f32),
            pltpu.VMEM((rows, rows), f32),
            pltpu.VMEM((KINDS * n_col, LANES), f32),
            pltpu.VMEM((KINDS * n_col, LANES), f32),
            pltpu.VMEM((3 * SIDE, KINDS * n_col, LANES), f32),
            dma((KINDS + 1,)),
            dma,
            dma,
            dma,
            dma,
            dma((4,)),
            dma,
            dma((N_SEM,)),
            dma,
        ],
        compiler_params=pltpu.CompilerParams(
            collective_id=0, has_side_effects=True, vmem_limit_bytes=36 * 2**20
        ),
        name="gather",
    )(*weights, gain.reshape(1, rows))
    tile = jax.ShapeDtypeStruct((n_col, LANES), f32)
    matrix = jax.ShapeDtypeStruct((n * rows, columns), bf16)
    q, k, v, tq, tk, tv = pl.pallas_call(
        store_kernel,
        out_shape=(matrix, matrix, matrix, tile, tile, tile),
        in_specs=[local, local],
        out_specs=(anywhere,) * 6,
        scratch_shapes=[dma, dma],
        compiler_params=pltpu.CompilerParams(vmem_limit_bytes=4 * 2**20),
        name="store",
    )(
        pltpu.with_memory_space_constraint(whole, pltpu.VMEM),
        pltpu.with_memory_space_constraint(factors, pltpu.VMEM),
    )
    return (q, k, v, tq.reshape(-1), tk.reshape(-1), tv.reshape(-1))


def solution(mesh):
    return jax.shard_map(
        on_device,
        mesh=mesh,
        in_specs=(P("fsdp", "model"),) * 9 + (P("fsdp"),),
        out_specs=(P(None, "model"),) * 3 + (P("model"),) * 3,
        check_vma=False,
    )
```

```python
import jax
import jax.numpy as jnp
from jax import lax
from jax.experimental import pallas as pl
from jax.experimental.pallas import tpu as pltpu
from jax.sharding import PartitionSpec as P

MESH = pl.DeviceIdType.MESH
D_MODEL = 4096
learn_rate = 0.2
hold_rate = 0.9

KINDS = 3
SIDE = 4
LANES = 128
QUARTER = 4


LAST = 2
EARLY = (((0, 16), (16, 8)), ((0, 8), (8, 16)))
EARLY_ROWS = 24
EARLY_NAMES = (("near", -1, 0), ("near", 1, 1))


def groups():
    taken = [EARLY_NAMES, (("near", -1, 1), ("near", 1, 0))]
    for first in (0, -1, 1, 2):
        if first == -1:
            taken.append((("far", 0, 0), ("far", 0, 1)))
        taken.append((("near2", first, -1, 0), ("near2", first, 1, 1)))
        taken.append((("near2", first, -1, 1), ("near2", first, 1, 0)))
        if first == 1:
            taken.append((("far2", 0, 0, 0), ("far2", 0, 0, 1)))
    for first in (-1, 1, LAST):
        taken.append((("far2", first, 0, 0), ("far2", first, 0, 1)))
    return taken


GROUPS = groups()
GROUP_OF = {name: k for k, names in enumerate(GROUPS) for name in names}
LAST_PARTS = ((0, 1, 0, 8), (1, 2, 0, 8), (2, 3, 0, 4), (2, 3, 4, 4))
WHOLE = (0, KINDS, 0, 8)
N_SEM = len(GROUPS) + len(LAST_PARTS) - 1
N_LINK = 4 * len(GROUPS)
N_PAIR = N_LINK + 4


def gather_kernel(
    wq, fq, sq, wk, fk, sk, wv, fv, sv, gain_ref,
    out, factor_ref,
    staged, gained, early, gain_row, gain_full, sums, row_sums, every,
    in_sem, sum_send, row_recv, column_recv, early_send, early_recv, all_send, link_recv, d2d_recv,
):
    me = lax.axis_index("fsdp")
    core = lax.rem(me, 2)
    chip = me // 2
    x = lax.rem(chip, SIDE)
    y = chip // SIDE
    rows = gained.shape[1]
    columns = gained.shape[2]
    n_col = columns // LANES
    piece = rows // QUARTER

    ys = [lax.rem(y + d, SIDE) * (2 * SIDE) for d in range(SIDE)]
    xs = [lax.rem(x + d, SIDE) * 2 for d in range(SIDE)]
    table = [[ys[dy] + xs[dx] + core for dx in range(SIDE)] for dy in range(SIDE)]

    def device(dy, dx, on=None):
        here = table[dy % SIDE][dx % SIDE]
        return here if on is None else here - core + on

    partner = me + 1 - 2 * core
    row_peers = [device(0, dx, on) for dx in (2, 1, 3) for on in (0, 1)] + [partner]
    column_peers = [device(dy, 0, on) for dy in (2, 1, 3) for on in (0, 1)]

    def wait_all(ref, sem):
        pltpu.make_async_copy(ref, ref, sem).wait()

    weights = (wq, fq, sq, wk, fk, sk, wv, fv, sv)
    gain_load = pltpu.make_async_copy(gain_ref, gain_row, in_sem.at[KINDS])
    gain_load.start()
    for k, ref in enumerate(weights):
        pltpu.make_async_copy(ref, staged.at[k], in_sem.at[k // 3]).start()

    barrier = pltpu.get_barrier_semaphore()
    for peer in column_peers + row_peers:
        pl.semaphore_signal(barrier, inc=1, device_id={"fsdp": peer}, device_id_type=MESH)

    gain_load.wait()
    gain_full[...] = jnp.broadcast_to(gain_row[...], (rows, rows)).T
    for m in range(KINDS):
        all_three = staged.at[3 * m : 3 * m + 3]
        pltpu.make_async_copy(all_three, all_three, in_sem.at[m]).wait()
        for j in range(n_col):
            at = slice(j * LANES, (j + 1) * LANES)
            hold = hold_rate * staged[3 * m + 1, :, at] + staged[3 * m + 2, :, at]
            latest = staged[3 * m, :, at] - learn_rate * hold
            value = latest * gain_full[...]
            gained[m, :, at] = value
            sums[m * n_col + j : m * n_col + j + 1, :] = jnp.sum(jnp.abs(value), axis=0, keepdims=True)

    pl.semaphore_wait(barrier, len(row_peers) + len(column_peers))

    def neighbour(color, stage, sign):
        along_x = (color == 0) == (stage == 1)
        return device(0, sign) if along_x else device(sign, 0)

    part = EARLY_ROWS

    def early_copy(color, side, k):
        start, count = EARLY[color][k]
        low = (2 * color + side) * piece + start
        return pltpu.make_async_remote_copy(
            src_ref=gained.at[:, low : low + count, :],
            dst_ref=early.at[color, side, :, start : start + count, :],
            send_sem=early_send,
            recv_sem=early_recv.at[2 * color + k],
            device_id={"fsdp": neighbour(color, 1, 1 - 2 * side)},
            device_id_type=MESH,
        )

    def sum_copy(source, slot, recv_sem, target):
        return pltpu.make_async_remote_copy(
            src_ref=source,
            dst_ref=every.at[slot],
            send_sem=sum_send,
            recv_sem=recv_sem,
            device_id={"fsdp": target},
            device_id_type=MESH,
        )

    n_row = 2 * SIDE
    hub = 1
    for dx in (2, 1, 3):
        sum_copy(sums, 2 * x + core, row_recv, device(0, dx, hub)).start()

    @pl.when(core != hub)
    def _():
        sum_copy(sums, 2 * x + core, row_recv, partner).start()

    for color in (1, 0):
        for side in (0, 1):
            early_copy(color, side, 0).start()

    @pl.when(core == hub)
    def _():
        every[2 * x + core] = sums[...]
        wait_all(every.at[0 : n_row - 1], row_recv)
        total = every[0]
        for k in range(1, n_row):
            total = total + every[k]
        row_sums[...] = total
        for peer in [*column_peers, partner]:
            sum_copy(row_sums, n_row + y, column_recv, peer).start()
        every[n_row + y] = total

    for color in (0, 1):
        for side in (0, 1):
            early_copy(color, side, 1).start()

    @pl.when(core == hub)
    def _():
        wait_all(every.at[n_row : n_row + SIDE - 1], column_recv)

    @pl.when(core != hub)
    def _():
        wait_all(every.at[n_row : n_row + SIDE], column_recv)

    total = every[n_row]
    for k in range(1, SIDE):
        total = total + every[n_row + k]
    factor_ref[...] = total / D_MODEL
    recip = 1.0 / factor_ref[...]

    def block_start(color, first, second):
        dy, dx = (second, first) if color == 0 else (first, second)
        return device(dy, dx) * rows

    both = (0, 1)

    def place(color, first, second, half, skip=0):
        at = block_start(color, first, second) + (2 * color + half) * piece + skip
        return out.at[:, pl.ds(pl.multiple_of(at, 8 if skip else piece), piece - skip), :]

    def where(color, name):
        if name[0] == "near":
            return name[1], 0
        if name[0] == "far":
            return 2, 0
        if name[0] == "near2":
            return name[1], name[2]
        return name[1], 2

    def cut(color, first, second, half, group):
        low, high, start, count = group
        at = block_start(color, first, second) + (2 * color + half) * piece + start * (piece // 8)
        rows_of = pl.ds(pl.multiple_of(at, 16), count * (piece // 8))
        return out.at[low:high, rows_of, :]

    def link(color, name, first, second, target, group):
        k = GROUP_OF[name]
        if name in EARLY_NAMES:
            ref = place(color, first, second, name[-1], part)
        elif group == WHOLE:
            ref = place(color, first, second, name[-1])
        else:
            ref = cut(color, first, second, name[-1], group)
            k += LAST_PARTS.index(group)
        return pltpu.make_async_remote_copy(
            src_ref=ref,
            dst_ref=ref,
            send_sem=all_send,
            recv_sem=link_recv.at[k],
            device_id={"fsdp": target},
            device_id_type=MESH,
        )

    def send(color, name, first, second, stage, sign):
        for group in LAST_PARTS if name[:2] == ("far2", LAST) else (WHOLE,):
            link(color, name, first, second, neighbour(color, stage, sign), group).start()

    def to_partner(color, first, second, half, group=WHOLE):
        ref = cut(color, first, second, half, group)
        pltpu.make_async_remote_copy(
            src_ref=ref,
            dst_ref=ref,
            send_sem=all_send,
            recv_sem=d2d_recv,
            device_id={"fsdp": partner},
            device_id_type=MESH,
        ).start()

    def arrived(color, name, group):
        first, second = where(color, name)
        half = name[-1]
        if name in EARLY_NAMES:
            send(color, ("far", 0, half), first, 0, 1, -first)
        if name[0] == "near":
            for to in (1, -1) if half == 0 else (-1, 1):
                send(color, ("near2", first, -to, half), first, 0, 2, to)
        if name[0] == "near2" and (name[2], half) in ((-1, 0), (1, 1)):
            send(color, ("far2", first, 0, half), first, second, 2, -name[2])

    def both_halves(first):
        for at in (0, 1):
            for to in (1, -1):
                half = at if to == 1 else 1 - at
                for color in both:
                    send(color, ("near2", first, -to, half), first, 0, 2, to)

    def take(k, group=WHOLE):
        low, high, _, count = group
        count = 4 * (piece - part if GROUPS[k] == EARLY_NAMES else count * (piece // 8))
        sem = link_recv.at[k if group == WHOLE else k + LAST_PARTS.index(group)]
        wait_all(out.at[low:high, 0:count, :], sem)
        for name in GROUPS[k]:
            for color in both:
                arrived(color, name, group)
        if GROUPS[k][0][0] == "far":
            both_halves(2)
        for name in GROUPS[k]:
            for color in both:
                to_partner(color, *where(color, name), name[-1], group)

    def scaled(color, first, half, source, low, count):
        start = block_start(color, first, 0) + (2 * color + half) * piece + low
        at = pl.multiple_of(start, 8)
        for m in range(KINDS):
            for j in range(n_col):
                cols = slice(j * LANES, (j + 1) * LANES)
                row = m * n_col + j
                out[m, pl.ds(at, count), cols] = (
                    source(m, cols) * recip[row : row + 1, :]
                ).astype(out.dtype)

    halves = (0, 1)
    def own(half, color, low, count):
        base = (2 * color + half) * piece + low
        scaled(color, 0, half, lambda m, cols: gained[m, base : base + count, cols], low, count)

    for same in (True, False):
        for half in halves:
            for color in both:
                if same:
                    own(half, color, part, piece - part)
                else:
                    own(half, color, 0, part)
        for half in halves:
            for color in both:
                to = 1 if (half == 0) == same else -1
                send(color, ("near", -to, half), 0, 0, 1, to)
    both_halves(0)
    for color in both:
        for k in range(2):
            start, count = EARLY[color][k]
            wait_all(early.at[color, :, :, start : start + count, :], early_recv.at[2 * color + k])
            for side in halves:
                rows_of = slice(start, start + count)
                scaled(
                    color, 2 * side - 1, side,
                    lambda m, cols: early[color, side, m, rows_of, cols], start, count,
                )
    for color in both:
        for half in halves:
            to_partner(color, 0, 0, half)

    for k in range(len(GROUPS) - 1):
        take(k)
    for group in LAST_PARTS:
        take(len(GROUPS) - 1, group)

    wait_all(out.at[:, 0 : N_PAIR * piece, :], d2d_recv)
    wait_all(out.at[:, 0 : (N_LINK + N_PAIR) * piece - 4 * part, :], all_send)
    wait_all(early, early_send)

    @pl.when(core == hub)
    def _():
        wait_all(every.at[0 : SIDE - 1 + len(column_peers) + 1], sum_send)

    @pl.when(core != hub)
    def _():
        wait_all(every.at[0:SIDE], sum_send)


def store_kernel(whole, factors, oq, ok, ov, tq, tk, tv, sem, small):
    n_row = oq.shape[0]
    parts = 8
    step = n_row // parts
    copies = []
    for m, ref in enumerate((oq, ok, ov)):
        for k in range(parts):
            copies.append(
                pltpu.make_async_copy(
                    whole.at[m, k * step : (k + 1) * step, :],
                    ref.at[k * step : (k + 1) * step, :],
                    sem,
                )
            )
    n_col = tq.shape[0]
    for m, ref in enumerate((tq, tk, tv)):
        copies.append(
            pltpu.make_async_copy(factors.at[m * n_col : (m + 1) * n_col, :], ref, small)
        )
    for copy in copies:
        copy.start()
    pltpu.make_async_copy(whole, whole, sem).wait()
    pltpu.make_async_copy(factors, factors, small).wait()


def on_device(*args):
    weights, gain = args[:9], args[9]
    rows, columns = weights[0].shape
    n_col = columns // LANES
    n = lax.axis_size("fsdp")
    f32, bf16 = jnp.float32, jnp.bfloat16
    anywhere = pl.BlockSpec(memory_space=pl.ANY)
    local = pl.BlockSpec(memory_space=pltpu.VMEM)
    dma = pltpu.SemaphoreType.DMA
    whole, factors = pl.pallas_call(
        gather_kernel,
        out_shape=(
            pltpu.VMEM((KINDS, n * rows, columns), bf16),
            pltpu.VMEM((KINDS * n_col, LANES), f32),
        ),
        in_specs=[anywhere] * 10,
        out_specs=(local, local),
        scratch_shapes=[
            pltpu.VMEM((9, rows, columns), f32),
            pltpu.VMEM((KINDS, rows, columns), f32),
            pltpu.VMEM((2, 2, KINDS, EARLY_ROWS, columns), f32),
            pltpu.VMEM((1, rows), f32),
            pltpu.VMEM((rows, rows), f32),
            pltpu.VMEM((KINDS * n_col, LANES), f32),
            pltpu.VMEM((KINDS * n_col, LANES), f32),
            pltpu.VMEM((3 * SIDE, KINDS * n_col, LANES), f32),
            dma((KINDS + 1,)),
            dma,
            dma,
            dma,
            dma,
            dma((4,)),
            dma,
            dma((N_SEM,)),
            dma,
        ],
        compiler_params=pltpu.CompilerParams(
            collective_id=0, has_side_effects=True, vmem_limit_bytes=36 * 2**20
        ),
        name="gather",
    )(*weights, gain.reshape(1, rows))
    tile = jax.ShapeDtypeStruct((n_col, LANES), f32)
    matrix = jax.ShapeDtypeStruct((n * rows, columns), bf16)
    q, k, v, tq, tk, tv = pl.pallas_call(
        store_kernel,
        out_shape=(matrix, matrix, matrix, tile, tile, tile),
        in_specs=[local, local],
        out_specs=(anywhere,) * 6,
        scratch_shapes=[dma, dma],
        compiler_params=pltpu.CompilerParams(vmem_limit_bytes=4 * 2**20),
        name="store",
    )(
        pltpu.with_memory_space_constraint(whole, pltpu.VMEM),
        pltpu.with_memory_space_constraint(factors, pltpu.VMEM),
    )
    return (q, k, v, tq.reshape(-1), tk.reshape(-1), tv.reshape(-1))


def solution(mesh):
    return jax.shard_map(
        on_device,
        mesh=mesh,
        in_specs=(P("fsdp", "model"),) * 9 + (P("fsdp"),),
        out_specs=(P(None, "model"),) * 3 + (P("model"),) * 3,
        check_vma=False,
    )
```

```python
import jax
import jax.numpy as jnp
from jax import lax
from jax.experimental import pallas as pl
from jax.experimental.pallas import tpu as pltpu
from jax.sharding import PartitionSpec as P

MESH = pl.DeviceIdType.MESH
D_MODEL = 4096
learn_rate = 0.2
hold_rate = 0.9

KINDS = 3
SIDE = 4
LANES = 128
QUARTER = 4


LAST = 2
EARLY = (((0, 16), (16, 8)), ((0, 8), (8, 16)))
EARLY_ROWS = 24
EARLY_NAMES = (("near", -1, 0), ("near", 1, 1))


def groups():
    taken = [EARLY_NAMES, (("near", -1, 1), ("near", 1, 0))]
    for first in (0, -1, 1, 2):
        if first == -1:
            taken.append((("far", 0, 0), ("far", 0, 1)))
        taken.append((("near2", first, -1, 0), ("near2", first, 1, 1)))
        taken.append((("near2", first, -1, 1), ("near2", first, 1, 0)))
        if first == 1:
            taken.append((("far2", 0, 0, 0), ("far2", 0, 0, 1)))
    for first in (-1, 1, LAST):
        taken.append((("far2", first, 0, 0), ("far2", first, 0, 1)))
    return taken


GROUPS = groups()
GROUP_OF = {name: k for k, names in enumerate(GROUPS) for name in names}
LAST_PARTS = ((0, 1, 0, 8), (1, 2, 0, 8), (2, 3, 0, 4), (2, 3, 4, 4))
WHOLE = (0, KINDS, 0, 8)
N_SEM = len(GROUPS) + len(LAST_PARTS) - 1
N_LINK = 4 * len(GROUPS)
N_PAIR = N_LINK + 4


def gather_kernel(
    wq, fq, sq, wk, fk, sk, wv, fv, sv, gain_ref,
    out, factor_ref,
    staged, gained, early, gain_row, gain_full, sums, row_sums, every,
    in_sem, sum_send, row_recv, column_recv, early_send, early_recv, all_send, link_recv, d2d_recv,
):
    me = lax.axis_index("fsdp")
    core = lax.rem(me, 2)
    chip = me // 2
    x = lax.rem(chip, SIDE)
    y = chip // SIDE
    rows = gained.shape[1]
    columns = gained.shape[2]
    n_col = columns // LANES
    piece = rows // QUARTER

    ys = [lax.rem(y + d, SIDE) * (2 * SIDE) for d in range(SIDE)]
    xs = [lax.rem(x + d, SIDE) * 2 for d in range(SIDE)]
    table = [[ys[dy] + xs[dx] + core for dx in range(SIDE)] for dy in range(SIDE)]

    def device(dy, dx, on=None):
        here = table[dy % SIDE][dx % SIDE]
        return here if on is None else here - core + on

    partner = me + 1 - 2 * core
    row_peers = [device(0, dx, on) for dx in (2, 1, 3) for on in (0, 1)] + [partner]
    column_peers = [device(dy, 0, on) for dy in (2, 1, 3) for on in (0, 1)]

    def wait_all(ref, sem):
        pltpu.make_async_copy(ref, ref, sem).wait()

    weights = (wq, fq, sq, wk, fk, sk, wv, fv, sv)
    gain_load = pltpu.make_async_copy(gain_ref, gain_row, in_sem.at[KINDS])
    gain_load.start()
    for k, ref in enumerate(weights):
        pltpu.make_async_copy(ref, staged.at[k], in_sem.at[k // 3]).start()

    barrier = pltpu.get_barrier_semaphore()
    hub = 1

    def greet(peer):
        pl.semaphore_signal(barrier, inc=1, device_id={"fsdp": peer}, device_id_type=MESH)

    for dy, dx in ((2, 0), (0, 2)):
        greet(device(dy, dx, 1 - core))

        @pl.when(core == hub)
        def _():
            greet(device(dy, dx))

    for dy, dx in ((1, 0), (3, 0), (0, 1), (0, 3)):
        greet(device(dy, dx, 1 - core))
        greet(device(dy, dx))
    greet(partner)

    gain_load.wait()
    gain_full[...] = jnp.broadcast_to(gain_row[...], (rows, rows)).T
    for m in range(KINDS):
        all_three = staged.at[3 * m : 3 * m + 3]
        pltpu.make_async_copy(all_three, all_three, in_sem.at[m]).wait()
        for j in range(n_col):
            at = slice(j * LANES, (j + 1) * LANES)
            hold = hold_rate * staged[3 * m + 1, :, at] + staged[3 * m + 2, :, at]
            latest = staged[3 * m, :, at] - learn_rate * hold
            value = latest * gain_full[...]
            gained[m, :, at] = value
            sums[m * n_col + j : m * n_col + j + 1, :] = jnp.sum(jnp.abs(value), axis=0, keepdims=True)

    near_peers = len(row_peers) + len(column_peers) - 2

    @pl.when(core == hub)
    def _():
        pl.semaphore_wait(barrier, near_peers + 2)

    @pl.when(core != hub)
    def _():
        pl.semaphore_wait(barrier, near_peers)


    def neighbour(color, stage, sign):
        along_x = (color == 0) == (stage == 1)
        return device(0, sign) if along_x else device(sign, 0)

    part = EARLY_ROWS

    def early_copy(color, side, k):
        start, count = EARLY[color][k]
        low = (2 * color + side) * piece + start
        return pltpu.make_async_remote_copy(
            src_ref=gained.at[:, low : low + count, :],
            dst_ref=early.at[color, side, :, start : start + count, :],
            send_sem=early_send,
            recv_sem=early_recv.at[2 * color + k],
            device_id={"fsdp": neighbour(color, 1, 1 - 2 * side)},
            device_id_type=MESH,
        )

    def sum_copy(source, slot, recv_sem, target):
        return pltpu.make_async_remote_copy(
            src_ref=source,
            dst_ref=every.at[slot],
            send_sem=sum_send,
            recv_sem=recv_sem,
            device_id={"fsdp": target},
            device_id_type=MESH,
        )

    n_row = 2 * SIDE
    for dx in (2, 1, 3):
        sum_copy(sums, 2 * x + core, row_recv, device(0, dx, hub)).start()

    @pl.when(core != hub)
    def _():
        sum_copy(sums, 2 * x + core, row_recv, partner).start()

    for color in (1, 0):
        for side in (0, 1):
            early_copy(color, side, 0).start()

    @pl.when(core == hub)
    def _():
        every[2 * x + core] = sums[...]
        wait_all(every.at[0 : n_row - 1], row_recv)
        total = every[0]
        for k in range(1, n_row):
            total = total + every[k]
        row_sums[...] = total
        for peer in [*column_peers, partner]:
            sum_copy(row_sums, n_row + y, column_recv, peer).start()
        every[n_row + y] = total

    for color in (0, 1):
        for side in (0, 1):
            early_copy(color, side, 1).start()

    @pl.when(core == hub)
    def _():
        wait_all(every.at[n_row : n_row + SIDE - 1], column_recv)

    @pl.when(core != hub)
    def _():
        wait_all(every.at[n_row : n_row + SIDE], column_recv)

    total = every[n_row]
    for k in range(1, SIDE):
        total = total + every[n_row + k]
    factor_ref[...] = total / D_MODEL
    recip = 1.0 / factor_ref[...]

    def block_start(color, first, second):
        dy, dx = (second, first) if color == 0 else (first, second)
        return device(dy, dx) * rows

    both = (0, 1)

    def place(color, first, second, half, skip=0):
        at = block_start(color, first, second) + (2 * color + half) * piece + skip
        return out.at[:, pl.ds(pl.multiple_of(at, 8 if skip else piece), piece - skip), :]

    def where(color, name):
        if name[0] == "near":
            return name[1], 0
        if name[0] == "far":
            return 2, 0
        if name[0] == "near2":
            return name[1], name[2]
        return name[1], 2

    def cut(color, first, second, half, group):
        low, high, start, count = group
        at = block_start(color, first, second) + (2 * color + half) * piece + start * (piece // 8)
        rows_of = pl.ds(pl.multiple_of(at, 16), count * (piece // 8))
        return out.at[low:high, rows_of, :]

    def link(color, name, first, second, target, group):
        k = GROUP_OF[name]
        if name in EARLY_NAMES:
            ref = place(color, first, second, name[-1], part)
        elif group == WHOLE:
            ref = place(color, first, second, name[-1])
        else:
            ref = cut(color, first, second, name[-1], group)
            k += LAST_PARTS.index(group)
        return pltpu.make_async_remote_copy(
            src_ref=ref,
            dst_ref=ref,
            send_sem=all_send,
            recv_sem=link_recv.at[k],
            device_id={"fsdp": target},
            device_id_type=MESH,
        )

    def send(color, name, first, second, stage, sign):
        for group in LAST_PARTS if name[:2] == ("far2", LAST) else (WHOLE,):
            link(color, name, first, second, neighbour(color, stage, sign), group).start()

    def to_partner(color, first, second, half, group=WHOLE):
        ref = cut(color, first, second, half, group)
        pltpu.make_async_remote_copy(
            src_ref=ref,
            dst_ref=ref,
            send_sem=all_send,
            recv_sem=d2d_recv,
            device_id={"fsdp": partner},
            device_id_type=MESH,
        ).start()

    def arrived(color, name, group):
        first, second = where(color, name)
        half = name[-1]
        if name in EARLY_NAMES:
            send(color, ("far", 0, half), first, 0, 1, -first)
        if name[0] == "near":
            for to in (1, -1) if half == 0 else (-1, 1):
                send(color, ("near2", first, -to, half), first, 0, 2, to)
        if name[0] == "near2" and (name[2], half) in ((-1, 0), (1, 1)):
            send(color, ("far2", first, 0, half), first, second, 2, -name[2])

    def both_halves(first):
        for at in (0, 1):
            for to in (1, -1):
                half = at if to == 1 else 1 - at
                for color in both:
                    send(color, ("near2", first, -to, half), first, 0, 2, to)

    def take(k, group=WHOLE):
        low, high, _, count = group
        count = 4 * (piece - part if GROUPS[k] == EARLY_NAMES else count * (piece // 8))
        sem = link_recv.at[k if group == WHOLE else k + LAST_PARTS.index(group)]
        wait_all(out.at[low:high, 0:count, :], sem)
        for name in GROUPS[k]:
            for color in both:
                arrived(color, name, group)
        if GROUPS[k][0][0] == "far":
            both_halves(2)
        for name in GROUPS[k]:
            for color in both:
                to_partner(color, *where(color, name), name[-1], group)

    def scaled(color, first, half, source, low, count):
        start = block_start(color, first, 0) + (2 * color + half) * piece + low
        at = pl.multiple_of(start, 8)
        for m in range(KINDS):
            for j in range(n_col):
                cols = slice(j * LANES, (j + 1) * LANES)
                row = m * n_col + j
                out[m, pl.ds(at, count), cols] = (
                    source(m, cols) * recip[row : row + 1, :]
                ).astype(out.dtype)

    halves = (0, 1)
    def own(half, color, low, count):
        base = (2 * color + half) * piece + low
        scaled(color, 0, half, lambda m, cols: gained[m, base : base + count, cols], low, count)

    for same in (True, False):
        for half in halves:
            for color in both:
                if same:
                    own(half, color, part, piece - part)
                else:
                    own(half, color, 0, part)
        for half in halves:
            for color in both:
                to = 1 if (half == 0) == same else -1
                send(color, ("near", -to, half), 0, 0, 1, to)
    both_halves(0)
    for color in both:
        for k in range(2):
            start, count = EARLY[color][k]
            wait_all(early.at[color, :, :, start : start + count, :], early_recv.at[2 * color + k])
            for side in halves:
                rows_of = slice(start, start + count)
                scaled(
                    color, 2 * side - 1, side,
                    lambda m, cols: early[color, side, m, rows_of, cols], start, count,
                )
    for color in both:
        for half in halves:
            to_partner(color, 0, 0, half)

    for k in range(len(GROUPS) - 1):
        take(k)
    for group in LAST_PARTS:
        take(len(GROUPS) - 1, group)

    wait_all(out.at[:, 0 : N_PAIR * piece, :], d2d_recv)
    wait_all(out.at[:, 0 : (N_LINK + N_PAIR) * piece - 4 * part, :], all_send)
    wait_all(early, early_send)

    @pl.when(core == hub)
    def _():
        wait_all(every.at[0 : SIDE - 1 + len(column_peers) + 1], sum_send)

    @pl.when(core != hub)
    def _():
        wait_all(every.at[0:SIDE], sum_send)


def store_kernel(whole, factors, oq, ok, ov, tq, tk, tv, sem, small):
    n_row = oq.shape[0]
    parts = 8
    step = n_row // parts
    copies = []
    for m, ref in enumerate((oq, ok, ov)):
        for k in range(parts):
            copies.append(
                pltpu.make_async_copy(
                    whole.at[m, k * step : (k + 1) * step, :],
                    ref.at[k * step : (k + 1) * step, :],
                    sem,
                )
            )
    n_col = tq.shape[0]
    for m, ref in enumerate((tq, tk, tv)):
        copies.append(
            pltpu.make_async_copy(factors.at[m * n_col : (m + 1) * n_col, :], ref, small)
        )
    for copy in copies:
        copy.start()
    pltpu.make_async_copy(whole, whole, sem).wait()
    pltpu.make_async_copy(factors, factors, small).wait()


def on_device(*args):
    weights, gain = args[:9], args[9]
    rows, columns = weights[0].shape
    n_col = columns // LANES
    n = lax.axis_size("fsdp")
    f32, bf16 = jnp.float32, jnp.bfloat16
    anywhere = pl.BlockSpec(memory_space=pl.ANY)
    local = pl.BlockSpec(memory_space=pltpu.VMEM)
    dma = pltpu.SemaphoreType.DMA
    whole, factors = pl.pallas_call(
        gather_kernel,
        out_shape=(
            pltpu.VMEM((KINDS, n * rows, columns), bf16),
            pltpu.VMEM((KINDS * n_col, LANES), f32),
        ),
        in_specs=[anywhere] * 10,
        out_specs=(local, local),
        scratch_shapes=[
            pltpu.VMEM((9, rows, columns), f32),
            pltpu.VMEM((KINDS, rows, columns), f32),
            pltpu.VMEM((2, 2, KINDS, EARLY_ROWS, columns), f32),
            pltpu.VMEM((1, rows), f32),
            pltpu.VMEM((rows, rows), f32),
            pltpu.VMEM((KINDS * n_col, LANES), f32),
            pltpu.VMEM((KINDS * n_col, LANES), f32),
            pltpu.VMEM((3 * SIDE, KINDS * n_col, LANES), f32),
            dma((KINDS + 1,)),
            dma,
            dma,
            dma,
            dma,
            dma((4,)),
            dma,
            dma((N_SEM,)),
            dma,
        ],
        compiler_params=pltpu.CompilerParams(
            collective_id=0, has_side_effects=True, vmem_limit_bytes=36 * 2**20
        ),
        name="gather",
    )(*weights, gain.reshape(1, rows))
    tile = jax.ShapeDtypeStruct((n_col, LANES), f32)
    matrix = jax.ShapeDtypeStruct((n * rows, columns), bf16)
    q, k, v, tq, tk, tv = pl.pallas_call(
        store_kernel,
        out_shape=(matrix, matrix, matrix, tile, tile, tile),
        in_specs=[local, local],
        out_specs=(anywhere,) * 6,
        scratch_shapes=[dma, dma],
        compiler_params=pltpu.CompilerParams(vmem_limit_bytes=4 * 2**20),
        name="store",
    )(
        pltpu.with_memory_space_constraint(whole, pltpu.VMEM),
        pltpu.with_memory_space_constraint(factors, pltpu.VMEM),
    )
    return (q, k, v, tq.reshape(-1), tk.reshape(-1), tv.reshape(-1))


def solution(mesh):
    return jax.shard_map(
        on_device,
        mesh=mesh,
        in_specs=(P("fsdp", "model"),) * 9 + (P("fsdp"),),
        out_specs=(P(None, "model"),) * 3 + (P("model"),) * 3,
        check_vma=False,
    )
```

```python
import jax
import jax.numpy as jnp
from jax import lax
from jax.experimental import pallas as pl
from jax.experimental.pallas import tpu as pltpu
from jax.sharding import PartitionSpec as P

MESH = pl.DeviceIdType.MESH
D_MODEL = 4096
learn_rate = 0.2
hold_rate = 0.9

KINDS = 3
SIDE = 4
LANES = 128
QUARTER = 4


LAST = 2
EARLY = (((0, 16), (16, 8)), ((0, 8), (8, 16)))
EARLY_ROWS = 24
EARLY_NAMES = (("near", -1, 0), ("near", 1, 1))


def groups():
    taken = [EARLY_NAMES, (("near", -1, 1), ("near", 1, 0))]
    for first in (0, -1, 1, 2):
        if first == -1:
            taken.append((("far", 0, 0), ("far", 0, 1)))
        taken.append((("near2", first, -1, 0), ("near2", first, 1, 1)))
        taken.append((("near2", first, -1, 1), ("near2", first, 1, 0)))
        if first == 1:
            taken.append((("far2", 0, 0, 0), ("far2", 0, 0, 1)))
    for first in (-1, 1, LAST):
        taken.append((("far2", first, 0, 0), ("far2", first, 0, 1)))
    return taken


GROUPS = groups()
GROUP_OF = {name: k for k, names in enumerate(GROUPS) for name in names}
LAST_PARTS = ((0, 2, 0, 8), (2, 3, 0, 4), (2, 3, 4, 2), (2, 3, 6, 2))
WHOLE = (0, KINDS, 0, 8)
N_SEM = len(GROUPS) + len(LAST_PARTS) - 1
N_LINK = 4 * len(GROUPS)
N_PAIR = N_LINK + 4


def gather_kernel(
    wq, fq, sq, wk, fk, sk, wv, fv, sv, gain_ref,
    out, factor_ref,
    staged, gained, early, gain_row, gain_full, sums, row_sums, every,
    in_sem, sum_send, row_recv, column_recv, early_send, early_recv, all_send, link_recv, d2d_recv,
):
    me = lax.axis_index("fsdp")
    core = lax.rem(me, 2)
    chip = me // 2
    x = lax.rem(chip, SIDE)
    y = chip // SIDE
    rows = gained.shape[1]
    columns = gained.shape[2]
    n_col = columns // LANES
    piece = rows // QUARTER

    ys = [lax.rem(y + d, SIDE) * (2 * SIDE) for d in range(SIDE)]
    xs = [lax.rem(x + d, SIDE) * 2 for d in range(SIDE)]
    table = [[ys[dy] + xs[dx] + core for dx in range(SIDE)] for dy in range(SIDE)]

    def device(dy, dx, on=None):
        here = table[dy % SIDE][dx % SIDE]
        return here if on is None else here - core + on

    partner = me + 1 - 2 * core
    row_peers = [device(0, dx, on) for dx in (2, 1, 3) for on in (0, 1)] + [partner]
    column_peers = [device(dy, 0, on) for dy in (2, 1, 3) for on in (0, 1)]

    def wait_all(ref, sem):
        pltpu.make_async_copy(ref, ref, sem).wait()

    weights = (wq, fq, sq, wk, fk, sk, wv, fv, sv)
    gain_load = pltpu.make_async_copy(gain_ref, gain_row, in_sem.at[KINDS])
    gain_load.start()
    for k, ref in enumerate(weights):
        pltpu.make_async_copy(ref, staged.at[k], in_sem.at[k // 3]).start()

    barrier = pltpu.get_barrier_semaphore()
    for peer in column_peers + row_peers:
        pl.semaphore_signal(barrier, inc=1, device_id={"fsdp": peer}, device_id_type=MESH)

    gain_load.wait()
    gain_full[...] = jnp.broadcast_to(gain_row[...], (rows, rows)).T
    for m in range(KINDS):
        all_three = staged.at[3 * m : 3 * m + 3]
        pltpu.make_async_copy(all_three, all_three, in_sem.at[m]).wait()
        for j in range(n_col):
            at = slice(j * LANES, (j + 1) * LANES)
            hold = hold_rate * staged[3 * m + 1, :, at] + staged[3 * m + 2, :, at]
            latest = staged[3 * m, :, at] - learn_rate * hold
            value = latest * gain_full[...]
            gained[m, :, at] = value
            sums[m * n_col + j : m * n_col + j + 1, :] = jnp.sum(jnp.abs(value), axis=0, keepdims=True)

    pl.semaphore_wait(barrier, len(row_peers) + len(column_peers))

    def neighbour(color, stage, sign):
        along_x = (color == 0) == (stage == 1)
        return device(0, sign) if along_x else device(sign, 0)

    part = EARLY_ROWS

    def early_copy(color, side, k):
        start, count = EARLY[color][k]
        low = (2 * color + side) * piece + start
        return pltpu.make_async_remote_copy(
            src_ref=gained.at[:, low : low + count, :],
            dst_ref=early.at[color, side, :, start : start + count, :],
            send_sem=early_send,
            recv_sem=early_recv.at[2 * color + k],
            device_id={"fsdp": neighbour(color, 1, 1 - 2 * side)},
            device_id_type=MESH,
        )

    def sum_copy(source, slot, recv_sem, target):
        return pltpu.make_async_remote_copy(
            src_ref=source,
            dst_ref=every.at[slot],
            send_sem=sum_send,
            recv_sem=recv_sem,
            device_id={"fsdp": target},
            device_id_type=MESH,
        )

    n_row = 2 * SIDE
    hub = 1
    for dx in (2, 1, 3):
        sum_copy(sums, 2 * x + core, row_recv, device(0, dx, hub)).start()

    @pl.when(core != hub)
    def _():
        sum_copy(sums, 2 * x + core, row_recv, partner).start()

    for color in (1, 0):
        for side in (0, 1):
            early_copy(color, side, 0).start()

    @pl.when(core == hub)
    def _():
        every[2 * x + core] = sums[...]
        wait_all(every.at[0 : n_row - 1], row_recv)
        total = every[0]
        for k in range(1, n_row):
            total = total + every[k]
        row_sums[...] = total
        for peer in [*column_peers, partner]:
            sum_copy(row_sums, n_row + y, column_recv, peer).start()
        every[n_row + y] = total

    for color in (0, 1):
        for side in (0, 1):
            early_copy(color, side, 1).start()

    @pl.when(core == hub)
    def _():
        wait_all(every.at[n_row : n_row + SIDE - 1], column_recv)

    @pl.when(core != hub)
    def _():
        wait_all(every.at[n_row : n_row + SIDE], column_recv)

    total = every[n_row]
    for k in range(1, SIDE):
        total = total + every[n_row + k]
    factor_ref[...] = total / D_MODEL
    recip = 1.0 / factor_ref[...]

    def block_start(color, first, second):
        dy, dx = (second, first) if color == 0 else (first, second)
        return device(dy, dx) * rows

    both = (0, 1)

    def place(color, first, second, half, skip=0):
        at = block_start(color, first, second) + (2 * color + half) * piece + skip
        return out.at[:, pl.ds(pl.multiple_of(at, 8 if skip else piece), piece - skip), :]

    def where(color, name):
        if name[0] == "near":
            return name[1], 0
        if name[0] == "far":
            return 2, 0
        if name[0] == "near2":
            return name[1], name[2]
        return name[1], 2

    def cut(color, first, second, half, group):
        low, high, start, count = group
        at = block_start(color, first, second) + (2 * color + half) * piece + start * (piece // 8)
        rows_of = pl.ds(pl.multiple_of(at, 8), count * (piece // 8))
        return out.at[low:high, rows_of, :]

    def link(color, name, first, second, target, group):
        k = GROUP_OF[name]
        if name in EARLY_NAMES:
            ref = place(color, first, second, name[-1], part)
        elif group == WHOLE:
            ref = place(color, first, second, name[-1])
        else:
            ref = cut(color, first, second, name[-1], group)
            k += LAST_PARTS.index(group)
        return pltpu.make_async_remote_copy(
            src_ref=ref,
            dst_ref=ref,
            send_sem=all_send,
            recv_sem=link_recv.at[k],
            device_id={"fsdp": target},
            device_id_type=MESH,
        )

    def send(color, name, first, second, stage, sign):
        for group in LAST_PARTS if name[:2] == ("far2", LAST) else (WHOLE,):
            link(color, name, first, second, neighbour(color, stage, sign), group).start()

    def to_partner(color, first, second, half, group=WHOLE):
        ref = cut(color, first, second, half, group)
        pltpu.make_async_remote_copy(
            src_ref=ref,
            dst_ref=ref,
            send_sem=all_send,
            recv_sem=d2d_recv,
            device_id={"fsdp": partner},
            device_id_type=MESH,
        ).start()

    def arrived(color, name, group):
        first, second = where(color, name)
        half = name[-1]
        if name in EARLY_NAMES:
            send(color, ("far", 0, half), first, 0, 1, -first)
        if name[0] == "near":
            for to in (1, -1) if half == 0 else (-1, 1):
                send(color, ("near2", first, -to, half), first, 0, 2, to)
        if name[0] == "near2" and (name[2], half) in ((-1, 0), (1, 1)):
            send(color, ("far2", first, 0, half), first, second, 2, -name[2])

    def both_halves(first):
        for at in (0, 1):
            for to in (1, -1):
                half = at if to == 1 else 1 - at
                for color in both:
                    send(color, ("near2", first, -to, half), first, 0, 2, to)

    def take(k, group=WHOLE):
        low, high, _, count = group
        count = 4 * (piece - part if GROUPS[k] == EARLY_NAMES else count * (piece // 8))
        sem = link_recv.at[k if group == WHOLE else k + LAST_PARTS.index(group)]
        wait_all(out.at[low:high, 0:count, :], sem)
        for name in GROUPS[k]:
            for color in both:
                arrived(color, name, group)
        if GROUPS[k][0][0] == "far":
            both_halves(2)
        for name in GROUPS[k]:
            for color in both:
                to_partner(color, *where(color, name), name[-1], group)

    def scaled(color, first, half, source, low, count):
        start = block_start(color, first, 0) + (2 * color + half) * piece + low
        at = pl.multiple_of(start, 8)
        for m in range(KINDS):
            for j in range(n_col):
                cols = slice(j * LANES, (j + 1) * LANES)
                row = m * n_col + j
                out[m, pl.ds(at, count), cols] = (
                    source(m, cols) * recip[row : row + 1, :]
                ).astype(out.dtype)

    halves = (0, 1)
    def own(half, color, low, count):
        base = (2 * color + half) * piece + low
        scaled(color, 0, half, lambda m, cols: gained[m, base : base + count, cols], low, count)

    waiting = []

    def flush(keep):
        while len(waiting) > keep:
            color, half, to = waiting.pop(0)
            send(color, ("near", -to, half), 0, 0, 1, to)

    for same in (True, False):
        for half in halves:
            for color in both:
                if same:
                    own(half, color, part, piece - part)
                else:
                    own(half, color, 0, part)
                waiting.append((color, half, 1 if (half == 0) == same else -1))
                flush(1)
    flush(0)
    both_halves(0)
    for color in both:
        for k in range(2):
            start, count = EARLY[color][k]
            wait_all(early.at[color, :, :, start : start + count, :], early_recv.at[2 * color + k])
            for side in halves:
                rows_of = slice(start, start + count)
                scaled(
                    color, 2 * side - 1, side,
                    lambda m, cols: early[color, side, m, rows_of, cols], start, count,
                )
    for color in both:
        for half in halves:
            to_partner(color, 0, 0, half)

    for k in range(len(GROUPS) - 1):
        take(k)
    for group in LAST_PARTS:
        take(len(GROUPS) - 1, group)

    wait_all(out.at[:, 0 : N_PAIR * piece, :], d2d_recv)
    wait_all(out.at[:, 0 : (N_LINK + N_PAIR) * piece - 4 * part, :], all_send)
    wait_all(early, early_send)

    @pl.when(core == hub)
    def _():
        wait_all(every.at[0 : SIDE - 1 + len(column_peers) + 1], sum_send)

    @pl.when(core != hub)
    def _():
        wait_all(every.at[0:SIDE], sum_send)


def store_kernel(whole, factors, oq, ok, ov, tq, tk, tv, sem, small):
    n_row = oq.shape[0]
    parts = 8
    step = n_row // parts
    copies = []
    for m, ref in enumerate((oq, ok, ov)):
        for k in range(parts):
            copies.append(
                pltpu.make_async_copy(
                    whole.at[m, k * step : (k + 1) * step, :],
                    ref.at[k * step : (k + 1) * step, :],
                    sem,
                )
            )
    n_col = tq.shape[0]
    for m, ref in enumerate((tq, tk, tv)):
        copies.append(
            pltpu.make_async_copy(factors.at[m * n_col : (m + 1) * n_col, :], ref, small)
        )
    for copy in copies:
        copy.start()
    pltpu.make_async_copy(whole, whole, sem).wait()
    pltpu.make_async_copy(factors, factors, small).wait()


def on_device(*args):
    weights, gain = args[:9], args[9]
    rows, columns = weights[0].shape
    n_col = columns // LANES
    n = lax.axis_size("fsdp")
    f32, bf16 = jnp.float32, jnp.bfloat16
    anywhere = pl.BlockSpec(memory_space=pl.ANY)
    local = pl.BlockSpec(memory_space=pltpu.VMEM)
    dma = pltpu.SemaphoreType.DMA
    whole, factors = pl.pallas_call(
        gather_kernel,
        out_shape=(
            pltpu.VMEM((KINDS, n * rows, columns), bf16),
            pltpu.VMEM((KINDS * n_col, LANES), f32),
        ),
        in_specs=[anywhere] * 10,
        out_specs=(local, local),
        scratch_shapes=[
            pltpu.VMEM((9, rows, columns), f32),
            pltpu.VMEM((KINDS, rows, columns), f32),
            pltpu.VMEM((2, 2, KINDS, EARLY_ROWS, columns), f32),
            pltpu.VMEM((1, rows), f32),
            pltpu.VMEM((rows, rows), f32),
            pltpu.VMEM((KINDS * n_col, LANES), f32),
            pltpu.VMEM((KINDS * n_col, LANES), f32),
            pltpu.VMEM((3 * SIDE, KINDS * n_col, LANES), f32),
            dma((KINDS + 1,)),
            dma,
            dma,
            dma,
            dma,
            dma((4,)),
            dma,
            dma((N_SEM,)),
            dma,
        ],
        compiler_params=pltpu.CompilerParams(
            collective_id=0, has_side_effects=True, vmem_limit_bytes=36 * 2**20
        ),
        name="gather",
    )(*weights, gain.reshape(1, rows))
    tile = jax.ShapeDtypeStruct((n_col, LANES), f32)
    matrix = jax.ShapeDtypeStruct((n * rows, columns), bf16)
    q, k, v, tq, tk, tv = pl.pallas_call(
        store_kernel,
        out_shape=(matrix, matrix, matrix, tile, tile, tile),
        in_specs=[local, local],
        out_specs=(anywhere,) * 6,
        scratch_shapes=[dma, dma],
        compiler_params=pltpu.CompilerParams(vmem_limit_bytes=4 * 2**20),
        name="store",
    )(
        pltpu.with_memory_space_constraint(whole, pltpu.VMEM),
        pltpu.with_memory_space_constraint(factors, pltpu.VMEM),
    )
    return (q, k, v, tq.reshape(-1), tk.reshape(-1), tv.reshape(-1))


def solution(mesh):
    return jax.shard_map(
        on_device,
        mesh=mesh,
        in_specs=(P("fsdp", "model"),) * 9 + (P("fsdp"),),
        out_specs=(P(None, "model"),) * 3 + (P("model"),) * 3,
        check_vma=False,
    )
```
